256 devices in a mesh: store: 4 (over x), row: 4 (over y_lo, core), col: 16 (over z, y_hi).
Axes of the slice: x: 4, y: 4 (y_hi: 2, y_lo: 2; y = y_hi * 2 + y_lo), z: 8, core: 2. Of those that a mesh axis runs over, the one named last changes fastest.
Arguments:
- tokens: bfloat16 [4096, 6144], P(('store', 'col'), 'row'), may hold values from -24 to 24
- ln_gain: bfloat16 [6144], P('row'), may hold values from 0.099609375 to 1.8984375
- qkv_weight: bfloat16 [6144, 3, 32, 128], P('row', None, 'col', 'store'), may hold values from -0.076546554 to 0.076546554
- q_gain: bfloat16 [128], replicated, may hold values from 0.5 to 7
- k_gain: bfloat16 [128], replicated, may hold values from 0.5 to 7
- out_weight: bfloat16 [32, 128, 6144], P('col', 'store', 'row'), may hold values from -0.09375 to 0.09375
- mlp_in: bfloat16 [6144, 12288], P('row', ('store', 'col')), may hold values from -0.078125 to 0.078125
- mlp_bias: bfloat16 [12288], P(('store', 'col')), may hold values from -3 to 3
- mlp_out: bfloat16 [12288, 6144], P(('store', 'col'), 'row'), may hold values from -0.0546875 to 0.0546875
- out_bias: bfloat16 [6144], P('row'), may hold values from -3 to 3
Outputs:
- mixed: float32 [4096, 6144], P(('store', 'col'), 'row')
The draws below stay inside these ranges and needn't reach their ends.
All inputs are finite; a program needn't handle non-finite values.
Results may differ from the reference program's by a relative error of at most 0.0059.
Values may be sent and summed in bfloat16 or wider, within the bound.
A program may use at most 64 MiB of HBM per device.

```python
import math
import jax
import jax.numpy as jnp
from jax import lax

D = 6144
HEADS = 32
HD = 128
FF = 12288
PATCHES = 256
TOKENS = 4096


def draw_tokens(key, part):
    subkeys = jax.random.split(key, 4)
    base_vals = jax.random.normal(subkeys[0], (TOKENS, D), jnp.float32)
    col_ramp = (1.0 + 2.0 * jnp.arange(D, dtype=jnp.float32) / D) / 2.0
    row_scale = jnp.exp(jax.random.uniform(subkeys[2], (TOKENS, 1), jnp.float32, math.log(0.3), math.log(3.0)))
    col_scale = jnp.exp(jax.random.uniform(subkeys[3], (1, D), jnp.float32, math.log(0.3), math.log(3.0)))
    values = base_vals * row_scale * col_scale * col_ramp[None, :]
    return jnp.clip(values, -24.0, 24.0).astype(jnp.bfloat16)


def draw_qkv_weight(key, part):
    subkeys = jax.random.split(jax.random.fold_in(key, 7), 1)
    limit = 6.0 * D ** (-0.5)
    values = jax.random.normal(subkeys[0], (D, 3, HEADS, HD), jnp.float32) * D ** (-0.5)
    return jnp.clip(values, -limit, limit).astype(jnp.bfloat16)


def draw_q_gain(key, part):
    values = jax.random.uniform(jax.random.fold_in(key, 11), (HD,), jnp.float32, 0.5, 2.5)
    return values.astype(jnp.bfloat16)


def draw_k_gain(key, part):
    values = jax.random.uniform(jax.random.fold_in(key, 13), (HD,), jnp.float32, 0.5, 2.5)
    return values.astype(jnp.bfloat16)


def block_levels(stream_key, extent, shards, smallest, high):
    def one(dim, parts):
        steps = jax.random.uniform(jax.random.fold_in(jax.random.fold_in(stream_key, 6), dim), (parts,), jnp.float32, smallest / len(shards), high / len(shards))
        return jnp.repeat(jnp.exp(steps), extent[dim] // parts).reshape((-1,) + (1,) * (len(extent) - dim - 1))

    loudness = one(*shards[0])
    for cut in shards[1:]:
        loudness = loudness * one(*cut)
    return loudness


def noise(own_key, extent, scale, reach, shards=(), kind=jnp.bfloat16):
    drawn = jax.random.normal(own_key, extent, jnp.float32) * scale
    if len(shards) > 0:
        drawn = block_levels(own_key, extent, shards, -0.22, 0.18) * drawn
    return jnp.clip(drawn, min=-reach, max=reach).astype(kind)


def setup_inputs(seed: int = 0) -> dict:
    splits = jax.random.split(jax.random.key(seed), 11)
    tokens = draw_tokens(jax.random.fold_in(splits[10], 71), 0)
    ln_gain = jnp.clip(1.0 + 0.18 * jax.random.normal(splits[1], (D,), jnp.float32), 0.099609375, 1.8984375).astype(jnp.bfloat16)
    qkv_weight = draw_qkv_weight(jax.random.fold_in(splits[10], 71), 0)
    q_gain = draw_q_gain(jax.random.fold_in(splits[10], 71), 0)
    k_gain = draw_k_gain(jax.random.fold_in(splits[10], 71), 0)
    out_weight = noise(splits[5], (HEADS, HD, D), (HEADS * HD) ** -0.5, 0.09375, ((0, 16), (1, 4), (2, 4)))
    mlp_in = noise(splits[6], (D, FF), D ** -0.5, 0.078125, ((0, 4), (1, 64)))
    mlp_bias = noise(splits[7], (FF,), 0.5, 3.0, ((0, 64),))
    mlp_out = noise(splits[8], (FF, D), FF ** -0.5, 0.0546875, ((0, 64), (1, 4)))
    out_bias = noise(splits[9], (D,), 0.5, 3.0, ((0, 4),))
    return {"tokens": tokens, "ln_gain": ln_gain, "qkv_weight": qkv_weight, "q_gain": q_gain, "k_gain": k_gain, "out_weight": out_weight, "mlp_in": mlp_in, "mlp_bias": mlp_bias, "mlp_out": mlp_out, "out_bias": out_bias}


epsilon = 1e-06

def head_norm(values, gain):
    average = lax.optimization_barrier(jnp.mean(values, -1, keepdims=True))
    centred = values - average
    spread = lax.optimization_barrier(jnp.mean(centred * centred, -1, keepdims=True))
    return (centred * lax.rsqrt(spread + epsilon) * gain.astype(jnp.float32)).astype(jnp.bfloat16)

def reference(tokens, ln_gain, qkv_weight, q_gain, k_gain, out_weight, mlp_in, mlp_bias, mlp_out, out_bias):
    tok_f32 = tokens.astype(jnp.float32)
    average = lax.optimization_barrier(jnp.mean(tok_f32, 1, keepdims=True))
    variance = lax.optimization_barrier(jnp.mean(tok_f32 * tok_f32, 1, keepdims=True)) - average * average
    normed = ((tok_f32 - average) * lax.rsqrt(variance + epsilon) * ln_gain.astype(jnp.float32)).astype(jnp.bfloat16)
    qkv_sum = jnp.dot(normed, qkv_weight.reshape(D, 3 * HEADS * HD), preferred_element_type=jnp.float32)
    shaped = qkv_sum.reshape(TOKENS // PATCHES, PATCHES, 3, HEADS, HD)

    def one_image(image_block):
        queries = head_norm(image_block[:, 0], q_gain)
        key_rows = head_norm(image_block[:, 1], k_gain)
        value_rows = image_block[:, 2].astype(jnp.bfloat16)
        scores = jnp.einsum('qhe,khe->hqk', queries.astype(jnp.float32), key_rows.astype(jnp.float32)) * HD ** (-0.5)
        highest = lax.optimization_barrier(jnp.max(scores, -1, keepdims=True))
        exponent = jnp.exp(scores - highest)
        softmax_w = (exponent / lax.optimization_barrier(jnp.sum(exponent, -1, keepdims=True))).astype(jnp.bfloat16)
        mixed_heads = jnp.einsum('hqk,khe->qhe', softmax_w.astype(jnp.float32), value_rows.astype(jnp.float32))
        return mixed_heads.astype(jnp.bfloat16)
    attended = lax.map(one_image, shaped).reshape(TOKENS, HEADS * HD)
    pre_hidden = jnp.dot(normed, mlp_in, preferred_element_type=jnp.float32) + mlp_bias.astype(jnp.float32)
    hidden = jax.nn.gelu(pre_hidden, approximate=False).astype(jnp.bfloat16)
    attn_out = jnp.dot(attended, out_weight.reshape(HEADS * HD, D), preferred_element_type=jnp.float32)
    mlp_result = jnp.dot(hidden, mlp_out, preferred_element_type=jnp.float32)
    return tok_f32 + attn_out + mlp_result + out_bias.astype(jnp.float32)
```

```python
import functools

import jax
import jax.numpy as jnp
from jax import lax
from jax.experimental import pallas as pl
from jax.experimental.pallas import tpu as pltpu
from jax.sharding import Mesh
from jax.sharding import PartitionSpec as P

D = 6144
HD = 128
IMAGE = 256
NX, NZ = 4, 8
BLOCK = 64
ROWS = 1024
PIECE = 1536
HALF = 768
UNITS = 96
EPS = 1e-06
MESH = pl.DeviceIdType.MESH
F32, BF16 = jnp.float32, jnp.bfloat16
NT = (((1,), (1,)), ((), ()))


class Names:
    def __init__(self):
        self.index = {}

    def __call__(self, *key):
        return self.index.setdefault(key, len(self.index))


N_SEMS = 224
N_LOCAL = 8


def kernel(
    tok, ln_gain, wq, wm, q_gain, k_gain, ow, bias, mo, out_bias,
    out,
    stats, stats_in, xg, WQ, WM, BI, OW, MO, hp, hx, att, part,
    zs, zr, ns, nr, ws, wr, send, recv, local,
):
    x, yl, k = lax.axis_index("x"), lax.axis_index("yl"), lax.axis_index("k")
    z, yh = lax.axis_index("z"), lax.axis_index("yh")
    nl, nk, nh = 1 - yl, 1 - k, 1 - yh
    xs = [lax.rem(x + d, NX) for d in range(NX)]
    zn = [lax.rem(z + d, NZ) for d in range(NZ)]
    at_x = lambda d: {"x": xs[d % NX]}
    at_z = lambda d: {"z": zn[d % NZ]}
    flip_l = {"yl": nl}
    flip_lh = {"yl": nl, "yh": nh}
    partner = {"k": nk}
    flip_lk = {"yl": nl, "k": nk}
    rel_l, rel_h = (yl, nl, nl, yl), (yh, yh, nh, nh)

    name, started = Names(), []

    def push(key, src, dst, peer):
        i = name(*key)
        copy = pltpu.make_async_remote_copy(
            src_ref=src, dst_ref=dst, send_sem=send.at[i], recv_sem=recv.at[i],
            device_id=peer, device_id_type=MESH,
        )
        copy.start()
        started.append(copy)

    def take(key, dst):
        i = name(*key)
        pltpu.make_async_remote_copy(
            src_ref=dst, dst_ref=dst, send_sem=send.at[i], recv_sem=recv.at[i],
            device_id=partner, device_id_type=MESH,
        ).wait_recv()

    barrier = pltpu.get_barrier_semaphore()
    peers = [at_x(1), at_x(-1), at_x(2), at_z(1), at_z(-1), flip_l, flip_lh, partner, flip_lk]
    for peer in peers:
        pl.semaphore_signal(barrier, inc=1, device_id=peer, device_id_type=MESH)

    t = tok[...].astype(F32)
    s1 = jnp.sum(t, 1, keepdims=True)
    s2 = jnp.sum(t * t, 1, keepdims=True)
    lane = lax.broadcasted_iota(jnp.int32, (BLOCK, 128), 1)
    stats[...] = jnp.where(lane < 64, s1, s2)
    pl.semaphore_wait(barrier, len(peers))

    def stored(w, j, c):
        if w == 0:
            return wq.at[:, j, :, c]
        return (None, wm, ow, mo)[w].at[j, :, c]

    def gathered(w, q, s, c):
        if w == 0:
            return WQ.at[q, :, s, :, c]
        return (None, WM, OW, MO)[w].at[q, s, :, c]

    full, halves = pl.ds(0, PIECE), (pl.ds(0, HALF), pl.ds(HALF, HALF))
    local_copies = []

    def x_push(w, q):
        qq = (yl, nl)[q]
        dst = gathered(w, qq, x, full)
        for d in (1, -1):
            push(("x", w, q, d), stored(w, yl, full) if q == 0 else dst, dst, at_x(d))

    def x_relay(w, q):
        qq = (yl, nl)[q]
        for d in (1, -1):
            take(("x", w, q, d), gathered(w, qq, xs[-d % NX], full))
            c = halves[0 if d == 1 else 1]
            ref = gathered(w, qq, xs[-d % NX], c)
            push(("x2", w, q, d), ref, ref, at_x(d))

    def x_last(w, q):
        qq = (yl, nl)[q]
        for d in (1, -1):
            c = halves[0 if d == 1 else 1]
            take(("x2", w, q, d), gathered(w, qq, xs[2], c))

    def w_send(w, h):
        push(("w", w, h), stored(w, nl, halves[h]), gathered(w, yl, x, halves[h]), flip_l)

    def w_take(w):
        for h in range(2):
            take(("w", w, h), gathered(w, nl, x, halves[h]))

    for i, peer in enumerate((partner, flip_l, flip_lk)):
        push(("stats", i), stats, stats_in.at[i], peer)
    x_push(0, 0)
    x_push(1, 0)
    w_send(0, 0)
    for d in (1, -1, 2):
        push(("bias", d), bias.at[yl], BI.at[x], at_x(d))
    for w in range(4):
        copy = pltpu.make_async_copy(stored(w, yl, full), gathered(w, yl, x, full), local.at[w])
        copy.start()
        local_copies.append(copy)
    BI[x] = bias[yl]

    for i in range(3):
        take(("stats", i), stats_in.at[i])
    total = stats[...] + stats_in[0] + stats_in[1] + stats_in[2]
    mean = total[:, 0:1] * (1.0 / D)
    var = total[:, 64:65] * (1.0 / D) - mean * mean
    normed = ((t - mean) * lax.rsqrt(var + EPS) * ln_gain[...].astype(F32)).astype(BF16)

    def tokens_at(h, r, zz):
        row = pl.multiple_of((zz * 2 + rel_h[r]) * BLOCK, BLOCK)
        return xg.at[h, rel_l[r], pl.ds(row, BLOCK)]

    def z_half(ref, d):
        return ref.at[pl.ds(0 if d == 1 else BLOCK // 2, BLOCK // 2)]

    own_row = pl.multiple_of((z * 2 + yh) * BLOCK, BLOCK)
    xg[0, yl, pl.ds(own_row, BLOCK)] = normed[:, :HALF]
    xg[1, yl, pl.ds(own_row, BLOCK)] = normed[:, HALF:]

    def z_push(h, r, d, dist):
        ref = tokens_at(h, r, zn[-d * (dist - 1) % NZ])
        if dist == 4:
            ref = z_half(ref, d)
        push(("z", h, r, d, dist), ref, ref, at_z(d))

    def z_take(h, r, d, dist):
        ref = tokens_at(h, r, zn[-d * dist % NZ])
        if dist == 4:
            ref = z_half(ref, d)
        take(("z", h, r, d, dist), ref)

    def y_push(h, dz):
        ref = tokens_at(h, 0, zn[dz % NZ])
        push(("yl", h, dz % NZ), ref, ref, flip_l)
        push(("yn", h, dz % NZ), ref, ref, flip_lh)

    def y_relay(h, dz):
        ref = tokens_at(h, 1, zn[dz % NZ])
        take(("yl", h, dz % NZ), ref)
        push(("yr", h, dz % NZ), ref, ref, flip_lh)

    def y_last(h, dz):
        take(("yn", h, dz % NZ), tokens_at(h, 2, zn[dz % NZ]))
        take(("yr", h, dz % NZ), tokens_at(h, 3, zn[dz % NZ]))

    def z_step(h, r, dist):
        for d in (1, -1):
            z_take(h, r, d, dist)
            if dist < 4:
                z_push(h, r, d, dist + 1)

    def z_first(h, r):
        for d in (1, -1):
            z_push(h, r, d, 1)

    z_first(0, 0)
    z_first(1, 0)
    y_push(1, 0)
    y_push(0, 0)
    w_send(0, 1)
    w_send(1, 0)

    z_step(0, 0, 1)
    y_relay(1, 0)
    z_first(1, 1)
    take(("yn", 1, 0), tokens_at(1, 2, z))
    z_first(1, 2)
    y_push(0, -1)
    y_push(0, 1)
    w_send(1, 1)
    x_relay(0, 0)
    y_relay(0, 0)
    take(("yr", 1, 0), tokens_at(1, 3, z))
    z_first(1, 3)
    w_take(0)
    x_push(0, 1)
    z_step(1, 0, 1)
    z_step(0, 0, 2)
    y_push(0, -2)
    y_push(0, 2)
    y_relay(0, -1)
    y_relay(0, 1)
    for r in (1, 2, 3):
        z_step(1, r, 1)
    x_relay(1, 0)
    w_take(1)
    x_push(1, 1)
    z_step(0, 0, 3)
    y_push(0, -3)
    y_push(0, 3)
    y_relay(0, -2)
    y_relay(0, 2)
    for r in range(4):
        z_step(1, r, 2)
    z_step(0, 0, 4)
    y_push(0, 4)
    x_relay(0, 1)
    y_relay(0, -3)
    y_relay(0, 3)
    for w in (2, 3):
        for h in range(2):
            w_send(w, h)
    for r in range(4):
        z_step(1, r, 3)
    x_relay(1, 1)
    x_push(2, 0)
    x_push(3, 0)
    y_relay(0, 4)
    for w in (0, 1):
        local_copies[w].wait()
        for q in range(2):
            x_last(w, q)
    for r in range(4):
        z_step(1, r, 4)
    for dz in (0, -1, 1, -2, 2, -3, 3, 4):
        y_last(0, dz)

    def project(i, carry):
        row = pl.multiple_of(lax.rem(i * 256 + nk * 512, ROWS), 256)
        acc_q = jnp.zeros((256, 384), F32)
        acc_m = jnp.zeros((256, 384), F32)
        for q in range(2):
            for h in range(2):
                lhs = xg[h, q, pl.ds(row, 256)]
                cols = slice(h * HALF, (h + 1) * HALF)
                acc_q += lax.dot_general(
                    lhs, WQ[q, :, :, :, cols].reshape(384, HALF), NT, preferred_element_type=F32
                )
                acc_m += lax.dot_general(
                    lhs, WM[q, :, :, cols].reshape(384, HALF), NT, preferred_element_type=F32
                )
        hp[pl.ds(row, 256), pl.ds(0, 384)] = acc_q
        hp[pl.ds(row, 256), pl.ds(384, 384)] = acc_m
        return carry

    lax.fori_loop(0, 2, project, 0)
    theirs = hp.at[pl.ds(pl.multiple_of(nk * 512, 512), 512)]
    push(("hx",), theirs, hx, partner)
    x_relay(2, 0)
    for w in (2, 3):
        w_take(w)
        x_push(w, 1)
    lax.fori_loop(2, 4, project, 0)
    x_relay(3, 0)
    take(("hx",), hx)
    for d in (1, -1, 2):
        take(("bias", d), BI.at[xs[-d % NX]])

    def head_norm(values, gain):
        centred = values - jnp.mean(values, -1, keepdims=True)
        spread = jnp.mean(centred * centred, -1, keepdims=True)
        return (centred * lax.rsqrt(spread + EPS) * gain[...].astype(F32)).astype(BF16)

    def image(i, carry):
        mine = pl.multiple_of(i * IMAGE, IMAGE)
        row = pl.multiple_of(k * 512 + mine, IMAGE)
        joined = hp[pl.ds(row, IMAGE)] + hx[pl.ds(mine, IMAGE)]
        q = head_norm(joined[:, 0:128], q_gain)
        kk = head_norm(joined[:, 128:256], k_gain)
        v = joined[:, 256:384].astype(BF16)
        scores = lax.dot_general(q, kk, NT, preferred_element_type=F32) * HD ** (-0.5)
        e = jnp.exp(scores - jnp.max(scores, -1, keepdims=True))
        probs = (e / jnp.sum(e, -1, keepdims=True)).astype(BF16)
        attended = jnp.dot(probs, v, preferred_element_type=F32)
        att[k, pl.ds(mine, IMAGE), pl.ds(0, 128)] = attended.astype(BF16)
        pre = joined[:, 384:768] + lax.dot_general(
            jnp.ones((IMAGE, 128), BF16), BI[...].reshape(384, 128), NT, preferred_element_type=F32
        )
        hidden = 0.5 * pre * (1.0 + lax.erf(pre * (0.5 ** 0.5)))
        att[k, pl.ds(mine, IMAGE), pl.ds(128, 384)] = hidden.astype(BF16)
        return carry

    lax.fori_loop(0, 2, image, 0)
    push(("att",), att.at[k], att.at[k], partner)
    for w in (2, 3):
        x_relay(w, 1)
    for w in (2, 3):
        local_copies[w].wait()
        for q in range(2):
            x_last(w, q)

    def output_terms(i, carry):
        row = pl.multiple_of(lax.rem(i * 256 + k * 512, ROWS), 256)
        a = att[row // 512, pl.ds(pl.multiple_of(lax.rem(row, 512), 256), 256)]
        for q in range(2):
            for h in range(2):
                cols = slice(h * HALF, (h + 1) * HALF)
                part[q, h, pl.ds(row, 256)] = jnp.dot(
                    a[:, :128], OW[q, :, :, cols].reshape(128, HALF), preferred_element_type=F32
                ) + jnp.dot(
                    a[:, 128:], MO[q, :, :, cols].reshape(384, HALF), preferred_element_type=F32
                )
        return carry

    lax.fori_loop(0, 2, output_terms, 0)
    take(("att",), att.at[nk])
    lax.fori_loop(2, 4, output_terms, 0)

    def term(h, r, dz):
        row = pl.multiple_of((zn[dz % NZ] * 2 + rel_h[r]) * BLOCK, BLOCK)
        return part.at[rel_l[r], h, pl.ds(row, BLOCK)]

    half = BLOCK // 2

    def chain(h, r, d, dist):
        g, di = (0 if h == 0 else 1 + r), (0 if d == 1 else 1)
        blk = term(h, r, d * dist)
        slot, landing = zs.at[g, di, dist - 1], zr.at[g, di, dist - 1]
        lo = 0 if d == 1 else half
        if dist == 4:
            slot, landing = slot.at[pl.ds(0, half)], landing.at[pl.ds(0, half)]
            slot[...] = blk[pl.ds(lo, half)].astype(BF16)
        elif dist == 3:
            before = zr.at[g, di, 3, pl.ds(0, half)]
            take(("c", g, d, 4), before)
            slot[pl.ds(half - lo, half)] = blk[pl.ds(half - lo, half)].astype(BF16)
            slot[pl.ds(lo, half)] = (blk[pl.ds(lo, half)] + before[...].astype(F32)).astype(BF16)
        else:
            before = zr.at[g, di, dist]
            take(("c", g, d, dist + 1), before)
            slot[...] = (blk[...] + before[...].astype(F32)).astype(BF16)
        push(("c", g, d, dist), slot, landing, at_z(d))

    def chains(h, r, dist):
        for d in (1, -1):
            chain(h, r, d, dist)

    def chain_end(h, r):
        g = 0 if h == 0 else 1 + r
        for d in (1, -1):
            take(("c", g, d, 1), zr.at[g, 0 if d == 1 else 1, 0])
        blk = term(h, r, 0)
        blk[...] = blk[...] + zr[g, 0, 0].astype(F32) + zr[g, 1, 0].astype(F32)

    def y_out(h, dz):
        g = dz % NZ if h == 0 else NZ
        for j, r in enumerate((2, 3)):
            ns[g, j] = term(h, r, dz)[...].astype(BF16)
            push(("n", g, j), ns.at[g, j], nr.at[g, j], flip_lh)

    def y_mid(h, dz):
        g = dz % NZ if h == 0 else NZ
        take(("n", g, 1), nr.at[g, 1])
        ws[g] = (term(h, 1, dz)[...] + nr[g, 1].astype(F32)).astype(BF16)
        push(("m", g), ws.at[g], wr.at[g], flip_l)

    def y_end(h, dz):
        g = dz % NZ if h == 0 else NZ
        take(("n", g, 0), nr.at[g, 0])
        take(("m", g), wr.at[g])
        blk = term(h, 0, dz)
        blk[...] = blk[...] + nr[g, 0].astype(F32) + wr[g].astype(F32)

    order = (4, 3, -3, 2, -2, 1, -1, 0)
    for r in range(4):
        chains(1, r, 4)
        y_out(0, order[r])
    for dz in order[4:]:
        y_out(0, dz)
    y_mid(0, 4)
    for r in range(4):
        chains(1, r, 3)
    y_mid(0, 3)
    y_mid(0, -3)
    y_end(0, 4)
    chains(0, 0, 4)
    for r in range(4):
        chains(1, r, 2)
    y_mid(0, 2)
    y_end(0, 3)
    y_end(0, -3)
    chains(0, 0, 3)
    y_mid(0, -2)
    for r in (2, 3, 1, 0):
        chains(1, r, 1)
    y_mid(0, 1)
    y_end(0, 2)
    y_end(0, -2)
    chains(0, 0, 2)
    y_mid(0, -1)
    chain_end(1, 2)
    chain_end(1, 3)
    y_out(1, 0)
    y_mid(0, 0)
    chain_end(1, 1)
    y_mid(1, 0)
    y_end(0, 1)
    y_end(0, -1)
    chains(0, 0, 1)
    chain_end(1, 0)
    y_end(0, 0)
    chain_end(0, 0)
    y_end(1, 0)
    for h in range(2):
        cols = slice(h * HALF, (h + 1) * HALF)
        out[:, cols] = tok[:, cols].astype(F32) + term(h, 0, 0)[...] + out_bias[:, cols].astype(F32)

    for copy in started:
        copy.wait_send()
    assert len(name.index) <= N_SEMS, len(name.index)


def per_device(
    tokens, ln_gain, qkv_weight, q_gain, k_gain, out_weight, mlp_in, mlp_bias, mlp_out, out_bias
):
    wq = jnp.transpose(qkv_weight, (1, 2, 3, 0))
    wm = jnp.transpose(mlp_in).reshape(2, UNITS, PIECE)
    mo = mlp_out.reshape(2, UNITS, PIECE)
    column0 = jnp.arange(128) == 0
    bias = jnp.where(column0, mlp_bias.reshape(2, UNITS, 1), 0).astype(BF16)
    vm, hbm = pl.BlockSpec(memory_space=pltpu.VMEM), pl.BlockSpec(memory_space=pl.ANY)
    block = (BLOCK, HALF)
    return pl.pallas_call(
        kernel,
        out_shape=jax.ShapeDtypeStruct((BLOCK, PIECE), F32),
        in_specs=[vm, vm, hbm, hbm, vm, vm, hbm, vm, hbm, vm],
        out_specs=vm,
        scratch_shapes=[
            pltpu.VMEM((BLOCK, 128), F32),
            pltpu.VMEM((3, BLOCK, 128), F32),
            pltpu.VMEM((2, 2, ROWS, HALF), BF16),
            pltpu.VMEM((2, 3, NX, 32, PIECE), BF16),
            pltpu.VMEM((2, NX, UNITS, PIECE), BF16),
            pltpu.VMEM((NX, UNITS, 128), BF16),
            pltpu.VMEM((2, NX, 32, PIECE), BF16),
            pltpu.VMEM((2, NX, UNITS, PIECE), BF16),
            pltpu.VMEM((ROWS, HALF), F32),
            pltpu.VMEM((512, HALF), F32),
            pltpu.VMEM((2, 512, 512), BF16),
            pltpu.VMEM((2, 2, ROWS, HALF), F32),
            pltpu.VMEM((5, 2, 4, *block), BF16),
            pltpu.VMEM((5, 2, 4, *block), BF16),
            pltpu.VMEM((NZ + 1, 2, *block), BF16),
            pltpu.VMEM((NZ + 1, 2, *block), BF16),
            pltpu.VMEM((NZ + 1, *block), BF16),
            pltpu.VMEM((NZ + 1, *block), BF16),
            pltpu.SemaphoreType.DMA((N_SEMS,)),
            pltpu.SemaphoreType.DMA((N_SEMS,)),
            pltpu.SemaphoreType.DMA((N_LOCAL,)),
        ],
        compiler_params=pltpu.CompilerParams(
            collective_id=0, has_side_effects=True, vmem_limit_bytes=62 * 1024 * 1024
        ),
        name="layer",
    )(
        tokens, ln_gain.reshape(1, PIECE), wq, wm, q_gain.reshape(1, HD), k_gain.reshape(1, HD),
        out_weight, bias, mo, out_bias.reshape(1, PIECE),
    )


def solution(mesh):
    split = Mesh(
        mesh.devices.reshape(NX, 2, 2, NZ, 2), ("x", "yl", "k", "z", "yh")
    )
    token_axes, row, col = ("x", "z", "yh"), ("yl", "k"), ("z", "yh")
    placed = (
        P(token_axes, row),
        P(row),
        P(row, None, col, "x"),
        P(),
        P(),
        P(col, "x", row),
        P(row, token_axes),
        P(token_axes),
        P(token_axes, row),
        P(row),
    )
    return jax.shard_map(
        per_device, mesh=split, in_specs=placed, out_specs=P(token_axes, row), check_vma=False
    )
```

```python
import jax
import jax.numpy as jnp
from jax import lax
from jax.experimental import pallas as pl
from jax.experimental.pallas import tpu as pltpu
from jax.sharding import Mesh
from jax.sharding import PartitionSpec as P

D = 6144
HD = 128
IMAGE = 256
NX, NZ = 4, 8
BLOCK = 64
ROWS = 1024
PIECE = 1536
HALF = 768
UNITS = 96
EPS = 1e-06
MESH = pl.DeviceIdType.MESH
F32, BF16 = jnp.float32, jnp.bfloat16
NT = (((1,), (1,)), ((), ()))


CHUNKS = (("z", 0, 256), ("y", 256, 512), ("z", 768, 512), ("y", 1280, 256))
N_SEMS = 320
LINK_RATE, LATENCY, ISSUE = 46.5e3, 2.3, 0.03


class Task:
    def __init__(self, name, takes=(), deps=(), work=0.02, body=None, pushes=(), prio=0.0):
        self.name, self.takes, self.deps, self.work = name, list(takes), list(deps), work
        self.body, self.pushes, self.prio = body, list(pushes), prio


def in_order(tasks):
    now, arrival, free, done, order, left = 0.0, {}, {}, set(), [], list(tasks)
    while left:
        best = None
        for task in left:
            if all(d in done for d in task.deps) and all(k in arrival for k, _ in task.takes):
                ready = max([now] + [arrival[k] for k, _ in task.takes])
                if best is None or (ready, task.prio) < best[:2]:
                    best = (ready, task.prio, task)
        now, _, task = best
        now += task.work
        for key, link, size, _ in task.pushes:
            now += ISSUE
            free[link] = max(now, free.get(link, 0.0)) + size / LINK_RATE
            arrival[key] = free[link] + LATENCY
        done.add(task.name)
        order.append(task)
        left.remove(task)
    return order


def kernel(
    tok_hbm, ln_gain, wq, wm, q_gain, k_gain, ow, bias_in, mo,
    out,
    tok, stats, stats_in, xg, WQ, WM, BV, BI, OW, MO, hp, hx, att, part, *rest,
):
    chunk_refs, (send, recv, local) = rest[:-3], rest[-3:]
    x, yl, k = lax.axis_index("x"), lax.axis_index("yl"), lax.axis_index("k")
    z, yh = lax.axis_index("z"), lax.axis_index("yh")
    nl, nk, nh = 1 - yl, 1 - k, 1 - yh
    xs = [lax.rem(x + d, NX) for d in range(NX)]
    zn = [lax.rem(z + d, NZ) for d in range(NZ)]
    at_x = lambda d: {"x": xs[d % NX]}
    at_z = lambda d: {"z": zn[d % NZ]}
    flip_l, flip_lh = {"yl": nl}, {"yl": nl, "yh": nh}
    partner, flip_lk = {"k": nk}, {"yl": nl, "k": nk}
    rel_l, rel_h = (yl, nl, nl, yl), (yh, yh, nh, nh)

    index, started = {}, []

    def push(key, src, dst, peer):
        i = index.setdefault(key, len(index))
        copy = pltpu.make_async_remote_copy(
            src_ref=src, dst_ref=dst, send_sem=send.at[i], recv_sem=recv.at[i],
            device_id=peer, device_id_type=MESH,
        )
        copy.start()
        started.append(copy)

    def take(key, dst):
        i = index.setdefault(key, len(index))
        pltpu.make_async_remote_copy(
            src_ref=dst, dst_ref=dst, send_sem=send.at[i], recv_sem=recv.at[i],
            device_id=partner, device_id_type=MESH,
        ).wait_recv()

    tok_copy = pltpu.make_async_copy(tok_hbm, tok, local.at[4])
    tok_copy.start()
    barrier = pltpu.get_barrier_semaphore()
    peers = [at_x(1), at_x(-1), at_x(2), at_z(1), at_z(-1), flip_l, flip_lh, partner, flip_lk]
    for peer in peers:
        pl.semaphore_signal(barrier, inc=1, device_id=peer, device_id_type=MESH)

    tasks = []

    def task(*args, **kwargs):
        tasks.append(Task(*args, **kwargs))

    def cols_of(w):
        return pl.ds(*CHUNKS[w[1]][1:]) if isinstance(w, tuple) else pl.ds(0, PIECE)

    def stored(w, j, c=None):
        c = cols_of(w) if c is None else c
        if w == "q":
            return wq.at[:, j, :, c]
        return {"i": wm, "o": ow, "m": mo}[w[0]].at[j, :, c]

    def gathered(w, q, s, c=None):
        c = cols_of(w) if c is None else c
        if w == "q":
            return WQ.at[q, :, s, :, c]
        return {"i": WM, "o": OW, "m": MO}[w[0]].at[q, s, :, c]

    def part_of(w, q, s, d):
        lo = 0 if d == 1 else 1
        if w in ("q", "i"):
            return gathered(w, q, s, pl.ds(lo * HALF, HALF))
        rows = 16 if w[0] == "o" else 48
        ref = OW if w[0] == "o" else MO
        return ref.at[q, s, pl.ds(lo * rows, rows), cols_of(w)]

    def bytes_of(w):
        width = CHUNKS[w[1]][2] if isinstance(w, tuple) else PIECE
        return (32 if w[0] == "o" else UNITS) * width * 2

    quarter = (yl, nl)

    def x_push(w, q):
        def refs(d):
            dst = gathered(w, quarter[q], x)
            return (stored(w, yl) if q == 0 else dst), dst, at_x(d)
        return [(("x", w, q, d), ("x", d), bytes_of(w), lambda d=d: refs(d)) for d in (1, -1)]

    def w_push(w, h=None):
        c = None if h is None else pl.ds(h * HALF, HALF)
        size = bytes_of(w) if h is None else bytes_of(w) // 2
        return (("w", w, h), "l", size, lambda: (stored(w, nl, c), gathered(w, yl, x, c), flip_l))

    def w_take(w, h=None):
        c = None if h is None else pl.ds(h * HALF, HALF)
        return (("w", w, h), lambda: gathered(w, nl, x, c))

    def x_relay(w, q, deps):
        for d in (1, -1):
            def refs(d=d):
                ref = part_of(w, quarter[q], xs[-d % NX], d)
                return ref, ref, at_x(d)
            task(
                ("x", w, q, d), deps=deps, prio=-1,
                takes=[(("x", w, q, d), lambda d=d: gathered(w, quarter[q], xs[-d % NX]))],
                pushes=[(("x2", w, q, d), ("x", d), bytes_of(w) // 2, refs)],
            )

    def x_last(w):
        return [
            (("x2", w, q, d), lambda q=q, d=d: part_of(w, quarter[q], xs[2], d))
            for q in range(2) for d in (1, -1)
        ]

    def stats_push(i, peer, link):
        return (("stats", i), link, BLOCK * 128 * 4, lambda: (stats, stats_in.at[i], peer))

    local_copies = []

    def begin():
        pl.semaphore_wait(barrier, len(peers))
        for i, w in enumerate(("q", "i")):
            copy = pltpu.make_async_copy(stored(w, yl), gathered(w, yl, x), local.at[i])
            copy.start()
            local_copies.append(copy)
        for i, (src, dst) in enumerate(((ow, OW), (mo, MO))):
            copy = pltpu.make_async_copy(src.at[yl], dst.at[yl, x], local.at[2 + i])
            copy.start()
            local_copies.append(copy)

    def statistics():
        tok_copy.wait()
        t = tok[...].astype(F32)
        s1 = jnp.sum(t, 1, keepdims=True)
        s2 = jnp.sum(t * t, 1, keepdims=True)
        lane = lax.broadcasted_iota(jnp.int32, (BLOCK, 128), 1)
        stats[...] = jnp.where(lane < 64, s1, s2)

    def bias_columns():
        b = bias_in[...].astype(F32)
        for i in range(2):
            BV[pl.ds(i * 128, 128), :] = jnp.broadcast_to(b[i : i + 1], (128, 128)).T.astype(BF16)
        mine = pl.ds(pl.multiple_of(yl * UNITS, 32), UNITS)
        BI[x] = BV[mine, :]

    def bias_refs(d):
        return BI.at[x], BI.at[x], at_x(d)

    def normalise():
        total = stats[...] + stats_in[0] + stats_in[1] + stats_in[2]
        mean = total[:, 0:1] * (1.0 / D)
        var = total[:, 64:65] * (1.0 / D) - mean * mean
        t = tok[...].astype(F32)
        g = ln_gain[...].astype(F32)
        g = jnp.concatenate([g[i : i + 1] for i in range(PIECE // 128)], axis=1)
        normed = ((t - mean) * lax.rsqrt(var + EPS) * g).astype(BF16)
        own_row = pl.multiple_of((z * 2 + yh) * BLOCK, BLOCK)
        xg[0, yl, pl.ds(own_row, BLOCK)] = normed[:, :HALF]
        xg[1, yl, pl.ds(own_row, BLOCK)] = normed[:, HALF:]

    size = BLOCK * HALF * 2

    def tokens_at(h, r, dz):
        row = pl.multiple_of((zn[dz % NZ] * 2 + rel_h[r]) * BLOCK, BLOCK)
        return xg.at[h, rel_l[r], pl.ds(row, BLOCK)]

    def z_half(ref, d):
        return ref.at[pl.ds(0 if d == 1 else BLOCK // 2, BLOCK // 2)]

    def z_ref(h, r, d, dist, back):
        ref = tokens_at(h, r, -d * (dist - back))
        return z_half(ref, d) if dist == 4 else ref

    def z_push(h, r, d, dist):
        def refs():
            ref = z_ref(h, r, d, dist, 1)
            return ref, ref, at_z(d)
        return (("z", h, r, d, dist), ("z", d), size // 2 if dist == 4 else size, refs)

    def z_take(h, r, d, dist):
        return (("z", h, r, d, dist), lambda: z_ref(h, r, d, dist, 0))

    def y_copy(kind, h, r, dz, link, peer):
        def refs():
            ref = tokens_at(h, r, dz)
            return ref, ref, peer
        return ((kind, h, dz % NZ), link, size, refs)

    def y_push(h, dz):
        return [y_copy("yl", h, 0, dz, "l", flip_l), y_copy("yn", h, 0, dz, "n", flip_lh)]

    def y_take(kind, h, dz):
        r = {"yl": 1, "yn": 2, "yr": 3}[kind]
        return ((kind, h, dz % NZ), lambda: tokens_at(h, r, dz))

    def z_first(h, r):
        return [z_push(h, r, d, 1) for d in (1, -1)]

    task(("begin",), body=begin, pushes=x_push("q", 0), work=0.0, prio=-100)
    task(
        ("stats",), deps=[("begin",)], body=statistics, work=1.0, prio=-99,
        pushes=[stats_push(0, partner, "k"), stats_push(1, flip_l, "l"), stats_push(2, flip_lk, "l")]
        + [w_push("q", 0)] + x_push("i", 0),
    )
    task(
        ("bias",), deps=[("stats",)], body=bias_columns, work=0.3, prio=-98,
        pushes=[(("bias", d), "b", 0, lambda d=d: bias_refs(d)) for d in (1, -1, 2)],
    )
    task(
        ("norm",), deps=[("bias",)], body=normalise, work=0.8, prio=-97,
        takes=[(("stats", i), lambda i=i: stats_in.at[i]) for i in range(3)],
        pushes=z_first(0, 0) + z_first(1, 0) + y_push(1, 0) + y_push(0, 0)
        + [w_push("q", 1), w_push("i", 0)],
    )
    gather = []
    for h in range(2):
        for r in range(1 if h == 0 else 4):
            for d in (1, -1):
                for dist in (1, 2, 3):
                    task(
                        ("z", h, r, d, dist), deps=[("norm",)], prio=0 if h == 0 else 5,
                        takes=[z_take(h, r, d, dist)],
                        pushes=[z_push(h, r, d, dist + 1)] + (y_push(0, -d * dist) if h == 0 else []),
                    )
    task(("z4",), takes=[z_take(0, 0, 1, 4), z_take(0, 0, -1, 4)], pushes=y_push(0, 4))
    for dz in range(NZ):
        task(
            ("yl", 0, dz), deps=[("norm",)], prio=1, takes=[y_take("yl", 0, dz)],
            pushes=[y_copy("yr", 0, 1, dz, "n", flip_lh)],
        )
    task(
        ("yl", 1, 0), deps=[("norm",)], prio=1, takes=[y_take("yl", 1, 0)],
        pushes=[y_copy("yr", 1, 1, 0, "n", flip_lh)] + z_first(1, 1),
    )
    task(("yn", 1, 0), deps=[("norm",)], prio=2, takes=[y_take("yn", 1, 0)], pushes=z_first(1, 2))
    task(("yr", 1, 0), deps=[("norm",)], prio=2, takes=[y_take("yr", 1, 0)], pushes=z_first(1, 3))
    task(("w", "i", 1), deps=[("z", 0, 0, 1, 1)], prio=3, pushes=[w_push("i", 1)])
    for w in ("q", "i"):
        task(
            ("w", w), deps=[("norm",)] + ([("w", "i", 1)] if w == "i" else []), prio=2,
            takes=[w_take(w, 0), w_take(w, 1)], pushes=x_push(w, 1),
        )
        x_relay(w, 0, [("norm",)])
        x_relay(w, 1, [("w", w)])
    n = len(CHUNKS)
    for c in range(n):
        pair = (("o", c), ("m", c))
        if c == 0:
            after = [("z", 0, 0, 1, 3), ("z", 0, 0, -1, 3)]
        else:
            after = [("w2s", c - 1)] + ([("w2p", c - 2)] if c >= 2 else [])
        task(("w2s", c), deps=after, prio=6, pushes=[w_push(w) for w in pair])
        if c == 0:
            after = [("x", "i", 0, 1), ("x", "i", 0, -1), ("w", "i"), ("x", "q", 1, 1), ("x", "q", 1, -1)]
        else:
            after = [("w2q", c - 1)] + ([("x", "i", 1, 1), ("x", "i", 1, -1)] if c == 1 else [])
        task(("w2p", c), deps=after, prio=7, pushes=x_push(pair[0], 0) + x_push(pair[1], 0))
        task(
            ("w2q", c), deps=[("w2s", c), ("w2p", c)], prio=7, takes=[w_take(w) for w in pair],
            pushes=x_push(pair[0], 1) + x_push(pair[1], 1),
        )
        for w in pair:
            x_relay(w, 0, [("w2p", c)])
            x_relay(w, 1, [("w2q", c)])
    first_relays = [t.name for t in tasks if t.name[0] in ("z", "z4", "yl", "yn", "yr", "w")]
    first_relays += [("x", w, q, d) for w in ("q", "i") for q in range(2) for d in (1, -1)]

    def project(i):
        row = pl.multiple_of(lax.rem(i * 256 + nk * 512, ROWS), 256)
        acc_q = jnp.zeros((256, 384), F32)
        acc_m = jnp.zeros((256, 384), F32)
        for q in range(2):
            for h in range(2):
                lhs = xg[h, q, pl.ds(row, 256)]
                cols = slice(h * HALF, (h + 1) * HALF)
                acc_q += lax.dot_general(
                    lhs, WQ[q, :, :, :, cols].reshape(384, HALF), NT, preferred_element_type=F32
                )
                acc_m += lax.dot_general(
                    lhs, WM[q, :, :, cols].reshape(384, HALF), NT, preferred_element_type=F32
                )
        hp[pl.ds(row, 256), pl.ds(0, 384)] = acc_q
        hp[pl.ds(row, 256), pl.ds(384, 384)] = acc_m

    def project_first():
        for copy in local_copies[:2]:
            copy.wait()
        project(0)

    def hx_refs(i):
        theirs = hp.at[pl.ds(pl.multiple_of(nk * 512 + i * 256, 256), 256)]
        return theirs, hx.at[pl.ds(i * 256, 256)], partner

    all_in = x_last("q") + x_last("i")
    all_in += [y_take(kind, 0, dz) for dz in range(NZ) for kind in ("yn", "yr")]
    all_in += [z_take(1, r, d, 4) for r in range(4) for d in (1, -1)]
    k_scale = LINK_RATE / 600e3
    for i in range(4):
        task(
            ("p", i), takes=all_in if i == 0 else [], deps=first_relays if i == 0 else [("p", i - 1)],
            body=project_first if i == 0 else (lambda i=i: project(i)), work=1.8, prio=10,
            pushes=[(("hx", i), "k", 256 * HALF * 4 * k_scale, lambda i=i: hx_refs(i))] if i < 2 else [],
        )

    def head_norm(values, gain):
        centred = values - jnp.mean(values, -1, keepdims=True)
        spread = jnp.mean(centred * centred, -1, keepdims=True)
        return (centred * lax.rsqrt(spread + EPS) * gain[...].astype(F32)).astype(BF16)

    def image(i):
        mine = pl.ds(i * IMAGE, IMAGE)
        row = pl.multiple_of(k * 512 + i * IMAGE, IMAGE)
        joined = hp[pl.ds(row, IMAGE)] + hx[mine]
        q = head_norm(joined[:, 0:128], q_gain)
        kk = head_norm(joined[:, 128:256], k_gain)
        v = joined[:, 256:384].astype(BF16)
        scores = lax.dot_general(q, kk, NT, preferred_element_type=F32) * HD ** (-0.5)
        e = jnp.exp(scores - jnp.max(scores, -1, keepdims=True))
        probs = (e / jnp.sum(e, -1, keepdims=True)).astype(BF16)
        attended = jnp.dot(probs, v, preferred_element_type=F32)
        att[k, mine, pl.ds(0, 128)] = attended.astype(BF16)
        unit = (lax.broadcasted_iota(jnp.int32, (IMAGE, 128), 1) == 0).astype(F32).astype(BF16)
        pre = joined[:, 384:768] + lax.dot_general(
            unit, BI[...].reshape(384, 128), NT, preferred_element_type=F32
        )
        hidden = 0.5 * pre * (1.0 + lax.erf(pre * (0.5 ** 0.5)))
        att[k, mine, pl.ds(128, 384)] = hidden.astype(BF16)

    def att_refs(i):
        ref = att.at[k, pl.ds(i * IMAGE, IMAGE)]
        return ref, ref, partner

    for i in range(2):
        takes = [(("hx", i), lambda i=i: hx.at[pl.ds(i * 256, 256)])]
        if i == 0:
            takes += [(("bias", d), lambda d=d: BI.at[xs[-d % NX]]) for d in (1, -1, 2)]
        task(
            ("image", i), takes=takes, deps=[("p", 3)] + [("image", 0)] * i, prio=10, work=0.8,
            body=lambda i=i: image(i),
            pushes=[(("att", i), "k", 256 * 512 * 2 * k_scale, lambda i=i: att_refs(i))],
        )

    def output_terms(c, half):
        if c == 0 and half == 0:
            for copy in local_copies[2:]:
                copy.wait()
        _, c0, width = CHUNKS[c]
        who = k if half == 0 else nk
        cols = slice(c0, c0 + width)
        for i in range(2):
            row = pl.multiple_of(who * 512 + i * 256, 256)
            a = att[who, pl.ds(i * 256, 256)]
            for q in range(2):
                part[q, pl.ds(row, 256), pl.ds(c0, width)] = jnp.dot(
                    a[:, :128], OW[q, :, :, cols].reshape(128, width), preferred_element_type=F32
                ) + jnp.dot(
                    a[:, 128:], MO[q, :, :, cols].reshape(384, width), preferred_element_type=F32
                )

    for c, (_, _, width) in enumerate(CHUNKS):
        pair = (("o", c), ("m", c))
        for half in range(2):
            deps = [("image", 1)]
            deps += [("x", w, q, d) for w in pair for q in range(2) for d in (1, -1)]
            deps += [("terms", c, 0)] if half else []
            deps += [("terms", c - 1, 1)] if c else []
            takes = (x_last(pair[0]) + x_last(pair[1])) if half == 0 else []
            if c == 0 and half == 1:
                takes = [
                    (("att", i), lambda i=i: att.at[nk, pl.ds(i * IMAGE, IMAGE)]) for i in range(2)
                ]
            task(
                ("terms", c, half), takes=takes, deps=deps, prio=9, work=1.44 * width / 768,
                body=lambda c=c, half=half: output_terms(c, half),
            )

    half = BLOCK // 2

    def term(c, r, dz):
        row = pl.multiple_of((zn[dz % NZ] * 2 + rel_h[r]) * BLOCK, BLOCK)
        return part.at[rel_l[r], pl.ds(row, BLOCK), pl.ds(*CHUNKS[c][1:])]

    def reduction(c):
        kind, _, width = CHUNKS[c]
        zs, zr, ns, nr, ms, mr = chunk_refs[6 * c : 6 * c + 6]
        block, groups = BLOCK * width * 2, (1 if kind == "y" else 4)
        work = 0.05 + 0.12 * width / HALF
        ready = ("terms", c, 1)

        def along_z(g, r, d, dist):
            slot, landing = zs.at[g, 0 if d == 1 else 1, dist - 1], zr.at[g, 0 if d == 1 else 1, dist - 1]
            if dist == 4:
                slot, landing = slot.at[pl.ds(0, half)], landing.at[pl.ds(0, half)]
            before = zr.at[g, 0 if d == 1 else 1, min(dist, 3)]
            if dist == 3:
                before = before.at[pl.ds(0, half)]
            lo = 0 if d == 1 else half

            def body():
                blk = term(c, r, d * dist)
                if dist == 4:
                    slot[...] = blk[pl.ds(lo, half)].astype(BF16)
                elif dist == 3:
                    slot[pl.ds(half - lo, half)] = blk[pl.ds(half - lo, half)].astype(BF16)
                    slot[pl.ds(lo, half)] = (
                        blk[pl.ds(lo, half)] + before[...].astype(F32)
                    ).astype(BF16)
                else:
                    slot[...] = (blk[...] + before[...].astype(F32)).astype(BF16)

            from_y = ("y_end", c, (d * dist) % NZ) if kind == "y" else ready
            prio = 3 if kind == "y" else 8 - dist * 0.5 + (0 if r in (2, 3) else 0.3)
            task(
                ("c", c, r, d, dist), body=body, work=work, prio=prio + c * 0.01,
                takes=[] if dist == 4 else [(("c", c, r, d, dist + 1), lambda: before)],
                deps=[from_y] + ([] if dist == 4 else [("c", c, r, d, dist + 1)]),
                pushes=[
                    (("c", c, r, d, dist), ("z", d), block // 2 if dist == 4 else block,
                     lambda: (slot, landing, at_z(d)))
                ],
            )

        def z_end(g, r):
            def body():
                blk = term(c, r, 0)
                blk[...] = blk[...] + zr[g, 0, 0].astype(F32) + zr[g, 1, 0].astype(F32)
            task(
                ("z_end", c, r), body=body, work=work, prio=2,
                takes=[(("c", c, r, d, 1), lambda i=i: zr.at[g, i, 0]) for i, d in enumerate((1, -1))],
                deps=[("c", c, r, d, 1) for d in (1, -1)] + ([("y_end", c, 0)] if kind == "y" else []),
            )

        def along_y(g, dz, deps_out, deps_mid, deps_end, prios):
            tree = (c + dz) % 2
            far, near = ((flip_lh, "n"), (flip_l, "l")) if tree == 0 else ((flip_l, "l"), (flip_lh, "n"))
            direct, mid = (2, 1) if tree == 0 else (1, 2)

            def out_body():
                for j, r in enumerate((direct, 3)):
                    ns[g, j] = term(c, r, dz)[...].astype(BF16)

            def mid_body():
                ms[g] = (term(c, mid, dz)[...] + nr[g, 1].astype(F32)).astype(BF16)

            def end_body():
                blk = term(c, 0, dz)
                blk[...] = blk[...] + nr[g, 0].astype(F32) + mr[g].astype(F32)

            task(
                ("y_out", c, dz), body=out_body, deps=deps_out(direct), prio=prios[0],
                work=0.05 + 0.15 * width / HALF,
                pushes=[
                    (("n", c, dz, j), far[1], block, lambda j=j: (ns.at[g, j], nr.at[g, j], far[0]))
                    for j in (1, 0)
                ],
            )
            task(
                ("y_mid", c, dz), body=mid_body, work=work, prio=prios[1],
                takes=[(("n", c, dz, 1), lambda: nr.at[g, 1])],
                deps=[("y_out", c, dz)] + deps_mid(mid),
                pushes=[(("m", c, dz), near[1], block, lambda: (ms.at[g], mr.at[g], near[0]))],
            )
            task(
                ("y_end", c, dz), body=end_body, work=work, prio=prios[2],
                takes=[(("n", c, dz, 0), lambda: nr.at[g, 0]), (("m", c, dz), lambda: mr.at[g])],
                deps=[("y_mid", c, dz)] + deps_end,
            )

        if kind == "y":
            for dz in range(NZ):
                far = min(dz, NZ - dz)
                along_y(
                    dz, dz, lambda r: [ready], lambda r: [], [],
                    (20 - far, 4 - far * 0.1, 5 - far * 0.1),
                )
        for g in range(groups):
            for d in (1, -1):
                for dist in (4, 3, 2, 1):
                    along_z(g, g, d, dist)
            z_end(g, g)
        if kind == "z":
            along_y(
                0, 0, lambda r: [("z_end", c, r), ("z_end", c, 3)], lambda r: [("z_end", c, r)],
                [("z_end", c, 0)], (1, 1, 1),
            )

    for c in range(n):
        reduction(c)

    for step in in_order(tasks):
        for key, ref in step.takes:
            take(key, ref())
        if step.body is not None:
            step.body()
        for key, _, _, refs in step.pushes:
            push(key, *refs())

    own = pl.ds(pl.multiple_of((z * 2 + yh) * BLOCK, BLOCK), BLOCK)
    out[...] = part[yl, own]
    for copy in started:
        copy.wait_send()
    assert len(index) <= N_SEMS, len(index)


def per_device(
    tokens, ln_gain, qkv_weight, q_gain, k_gain, out_weight, mlp_in, mlp_bias, mlp_out, out_bias
):
    wq = jnp.transpose(qkv_weight, (1, 2, 3, 0))
    wm = jnp.transpose(mlp_in).reshape(2, UNITS, PIECE)
    mo = mlp_out.reshape(2, UNITS, PIECE)
    bias = jnp.pad(mlp_bias, (0, 64)).reshape(2, 128)
    vm, hbm = pl.BlockSpec(memory_space=pltpu.VMEM), pl.BlockSpec(memory_space=pl.ANY)
    scratch = [
        pltpu.VMEM((BLOCK, PIECE), BF16),
        pltpu.VMEM((BLOCK, 128), F32),
        pltpu.VMEM((3, BLOCK, 128), F32),
        pltpu.VMEM((2, 2, ROWS, HALF), BF16),
        pltpu.VMEM((2, 3, NX, 32, PIECE), BF16),
        pltpu.VMEM((2, NX, UNITS, PIECE), BF16),
        pltpu.VMEM((256, 128), BF16),
        pltpu.VMEM((NX, UNITS, 128), BF16),
        pltpu.VMEM((2, NX, 32, PIECE), BF16),
        pltpu.VMEM((2, NX, UNITS, PIECE), BF16),
        pltpu.VMEM((ROWS, HALF), F32),
        pltpu.VMEM((512, HALF), F32),
        pltpu.VMEM((2, 512, 512), BF16),
        pltpu.VMEM((2, ROWS, PIECE), F32),
    ]
    for kind, _, width in CHUNKS:
        block = (BLOCK, width)
        groups, ys = (1, NZ) if kind == "y" else (4, 1)
        scratch += [pltpu.VMEM((groups, 2, 4, *block), BF16)] * 2
        scratch += [pltpu.VMEM((ys, 2, *block), BF16)] * 2
        scratch += [pltpu.VMEM((ys, *block), BF16)] * 2
    scratch += [
        pltpu.SemaphoreType.DMA((N_SEMS,)),
        pltpu.SemaphoreType.DMA((N_SEMS,)),
        pltpu.SemaphoreType.DMA((5,)),
    ]
    sums = pl.pallas_call(
        kernel,
        out_shape=jax.ShapeDtypeStruct((BLOCK, PIECE), F32),
        in_specs=[hbm, vm, hbm, hbm, vm, vm, hbm, vm, hbm],
        out_specs=vm,
        scratch_shapes=scratch,
        compiler_params=pltpu.CompilerParams(
            collective_id=0, has_side_effects=True, vmem_limit_bytes=60 * 1024 * 1024
        ),
        name="layer",
    )(
        tokens, ln_gain.reshape(PIECE // 128, 128), wq, wm, q_gain.reshape(1, HD),
        k_gain.reshape(1, HD), out_weight, bias, mo,
    )
    return tokens.astype(F32) + sums + out_bias.astype(F32)


def solution(mesh):
    split = Mesh(
        mesh.devices.reshape(NX, 2, 2, NZ, 2), ("x", "yl", "k", "z", "yh")
    )
    token_axes, row, col = ("x", "z", "yh"), ("yl", "k"), ("z", "yh")
    placed = (
        P(token_axes, row),
        P(row),
        P(row, None, col, "x"),
        P(),
        P(),
        P(col, "x", row),
        P(row, token_axes),
        P(token_axes),
        P(token_axes, row),
        P(row),
    )
    return jax.shard_map(
        per_device, mesh=split, in_specs=placed, out_specs=P(token_axes, row), check_vma=False
    )
```

```python
import jax
import jax.numpy as jnp
from jax import lax
from jax.experimental import pallas as pl
from jax.experimental.pallas import tpu as pltpu
from jax.sharding import Mesh
from jax.sharding import PartitionSpec as P

D = 6144
HD = 128
IMAGE = 256
NX, NZ = 4, 8
BLOCK = 64
ROWS = 1024
PIECE = 1536
HALF = 768
UNITS = 96
EPS = 1e-06
MESH = pl.DeviceIdType.MESH
F32, BF16 = jnp.float32, jnp.bfloat16
NT = (((1,), (1,)), ((), ()))


CHUNKS = (("z", 0, 256), ("y", 256, 512), ("z", 768, 512), ("y", 1280, 256))
N_SEMS = 320
LINK_RATE, LATENCY, ISSUE = 44e3, 2.3, 0.03


class Task:
    def __init__(self, name, takes=(), deps=(), work=0.02, body=None, pushes=(), prio=0.0):
        self.name, self.takes, self.deps, self.work = name, list(takes), list(deps), work
        self.body, self.pushes, self.prio = body, list(pushes), prio


def in_order(tasks):
    now, arrival, free, done, order, left = 0.0, {}, {}, set(), [], list(tasks)
    while left:
        best = None
        for task in left:
            if all(d in done for d in task.deps) and all(k in arrival for k, _ in task.takes):
                ready = max([now] + [arrival[k] for k, _ in task.takes])
                if best is None or (ready, task.prio) < best[:2]:
                    best = (ready, task.prio, task)
        now, _, task = best
        now += task.work
        for key, link, size, _ in task.pushes:
            now += ISSUE
            free[link] = max(now, free.get(link, 0.0)) + size / LINK_RATE
            arrival[key] = free[link] + LATENCY
        done.add(task.name)
        order.append(task)
        left.remove(task)
    return order


def kernel(
    tok_hbm, ln_gain, wq, wm, q_gain, k_gain, ow, bias_in, mo,
    out,
    tok, stats, stats_in, xg, WQ, WM, BV, BI, OW, MO, hq, hm, hxq, hxm, att, part, *rest,
):
    chunk_refs, (send, recv, local) = rest[:-3], rest[-3:]
    x, yl, k = lax.axis_index("x"), lax.axis_index("yl"), lax.axis_index("k")
    z, yh = lax.axis_index("z"), lax.axis_index("yh")
    nl, nk, nh = 1 - yl, 1 - k, 1 - yh
    xs = [lax.rem(x + d, NX) for d in range(NX)]
    zn = [lax.rem(z + d, NZ) for d in range(NZ)]
    at_x = lambda d: {"x": xs[d % NX]}
    at_z = lambda d: {"z": zn[d % NZ]}
    flip_l, flip_lh = {"yl": nl}, {"yl": nl, "yh": nh}
    partner, flip_lk = {"k": nk}, {"yl": nl, "k": nk}
    rel_l, rel_h = (yl, nl, nl, yl), (yh, yh, nh, nh)

    index, started = {}, []

    def push(key, src, dst, peer):
        i = index.setdefault(key, len(index))
        copy = pltpu.make_async_remote_copy(
            src_ref=src, dst_ref=dst, send_sem=send.at[i], recv_sem=recv.at[i],
            device_id=peer, device_id_type=MESH,
        )
        copy.start()
        started.append(copy)

    def take(key, dst):
        i = index.setdefault(key, len(index))
        pltpu.make_async_remote_copy(
            src_ref=dst, dst_ref=dst, send_sem=send.at[i], recv_sem=recv.at[i],
            device_id=partner, device_id_type=MESH,
        ).wait_recv()

    tok_copy = pltpu.make_async_copy(tok_hbm, tok, local.at[4])
    tok_copy.start()
    barrier = pltpu.get_barrier_semaphore()
    peers = [at_x(1), at_x(-1), at_x(2), at_z(1), at_z(-1), flip_l, flip_lh, partner, flip_lk]
    for peer in peers:
        pl.semaphore_signal(barrier, inc=1, device_id=peer, device_id_type=MESH)

    tasks = []

    def task(*args, **kwargs):
        tasks.append(Task(*args, **kwargs))

    def cols_of(w):
        return pl.ds(*CHUNKS[w[1]][1:]) if isinstance(w, tuple) else pl.ds(0, PIECE)

    def stored(w, j, c=None):
        c = cols_of(w) if c is None else c
        if w == "q":
            return wq.at[:, j, :, c]
        return {"i": wm, "o": ow, "m": mo}[w[0]].at[j, :, c]

    def gathered(w, q, s, c=None):
        c = cols_of(w) if c is None else c
        if w == "q":
            return WQ.at[q, :, s, :, c]
        return {"i": WM, "o": OW, "m": MO}[w[0]].at[q, s, :, c]

    def part_of(w, q, s, d):
        lo = 0 if d == 1 else 1
        if w in ("q", "i"):
            return gathered(w, q, s, pl.ds(lo * HALF, HALF))
        rows = 16 if w[0] == "o" else 48
        ref = OW if w[0] == "o" else MO
        return ref.at[q, s, pl.ds(lo * rows, rows), cols_of(w)]

    def bytes_of(w):
        width = CHUNKS[w[1]][2] if isinstance(w, tuple) else PIECE
        return (32 if w[0] == "o" else UNITS) * width * 2

    quarter = (yl, nl)

    def x_push(w, q):
        def refs(d):
            dst = gathered(w, quarter[q], x)
            return (stored(w, yl) if q == 0 else dst), dst, at_x(d)
        return [(("x", w, q, d), ("x", d), bytes_of(w), lambda d=d: refs(d)) for d in (1, -1)]

    def w_push(w, h=None):
        c = None if h is None else pl.ds(h * HALF, HALF)
        size = bytes_of(w) if h is None else bytes_of(w) // 2
        return (("w", w, h), "l", size, lambda: (stored(w, nl, c), gathered(w, yl, x, c), flip_l))

    def w_take(w, h=None):
        c = None if h is None else pl.ds(h * HALF, HALF)
        return (("w", w, h), lambda: gathered(w, nl, x, c))

    def x_relay(w, q, deps):
        for d in (1, -1):
            def refs(d=d):
                ref = part_of(w, quarter[q], xs[-d % NX], d)
                return ref, ref, at_x(d)
            task(
                ("x", w, q, d), deps=deps, prio=-1,
                takes=[(("x", w, q, d), lambda d=d: gathered(w, quarter[q], xs[-d % NX]))],
                pushes=[(("x2", w, q, d), ("x", d), bytes_of(w) // 2, refs)],
            )

    def x_last(w):
        return [
            (("x2", w, q, d), lambda q=q, d=d: part_of(w, quarter[q], xs[2], d))
            for q in range(2) for d in (1, -1)
        ]

    def stats_push(i, peer, link):
        return (("stats", i), link, 8 * 128 * 4, lambda: (stats, stats_in.at[i], peer))

    local_copies = []

    def begin():
        pl.semaphore_wait(barrier, len(peers))
        for i, w in enumerate(("q", "i")):
            copy = pltpu.make_async_copy(stored(w, yl), gathered(w, yl, x), local.at[i])
            copy.start()
            local_copies.append(copy)
        for i, (src, dst) in enumerate(((ow, OW), (mo, MO))):
            copy = pltpu.make_async_copy(src.at[yl], dst.at[yl, x], local.at[2 + i])
            copy.start()
            local_copies.append(copy)

    def statistics():
        tok_copy.wait()
        t = tok[...].astype(F32)
        s1 = jnp.sum(t, 1, keepdims=True)
        s2 = jnp.sum(t * t, 1, keepdims=True)
        lane = lax.broadcasted_iota(jnp.int32, (BLOCK, 128), 1)
        both = jnp.where(lane < 64, s1, s2)
        turned = jnp.concatenate([both, both], axis=0).T
        row = lax.broadcasted_iota(jnp.int32, (8, 128), 0)
        stats[...] = jnp.where(row < 4, turned[0:1], turned[64:65])

    def bias_columns():
        b = bias_in[...].astype(F32)
        for i in range(2):
            BV[pl.ds(i * 128, 128), :] = jnp.broadcast_to(b[i : i + 1], (128, 128)).T.astype(BF16)
        mine = pl.ds(pl.multiple_of(yl * UNITS, 32), UNITS)
        BI[x] = BV[mine, :]

    def bias_refs(d):
        return BI.at[x], BI.at[x], at_x(d)

    def normalise():
        total = stats[...] + stats_in[0] + stats_in[1] + stats_in[2]
        mean = total[0:1] * (1.0 / D)
        var = total[4:5] * (1.0 / D) - mean * mean
        row = lax.broadcasted_iota(jnp.int32, (128, 128), 0)
        turned = jnp.where(row < 64, mean, lax.rsqrt(var + EPS)).T
        mean, scale = turned[:BLOCK, 0:1], turned[:BLOCK, 64:65]
        t = tok[...].astype(F32)
        g = ln_gain[...].astype(F32)
        g = jnp.concatenate([g[i : i + 1] for i in range(PIECE // 128)], axis=1)
        normed = ((t - mean) * scale * g).astype(BF16)
        own_row = pl.multiple_of((z * 2 + yh) * BLOCK, BLOCK)
        xg[0, yl, pl.ds(own_row, BLOCK)] = normed[:, :HALF]
        xg[1, yl, pl.ds(own_row, BLOCK)] = normed[:, HALF:]

    size = BLOCK * HALF * 2

    def tokens_at(h, r, dz):
        row = pl.multiple_of((zn[dz % NZ] * 2 + rel_h[r]) * BLOCK, BLOCK)
        return xg.at[h, rel_l[r], pl.ds(row, BLOCK)]

    def z_half(ref, d):
        return ref.at[pl.ds(0 if d == 1 else BLOCK // 2, BLOCK // 2)]

    def z_ref(h, r, d, dist, back):
        ref = tokens_at(h, r, -d * (dist - back))
        return z_half(ref, d) if dist == 4 else ref

    def z_push(h, r, d, dist):
        def refs():
            ref = z_ref(h, r, d, dist, 1)
            return ref, ref, at_z(d)
        return (("z", h, r, d, dist), ("z", d), size // 2 if dist == 4 else size, refs)

    def z_take(h, r, d, dist):
        return (("z", h, r, d, dist), lambda: z_ref(h, r, d, dist, 0))

    def y_copy(kind, h, r, dz, link, peer):
        def refs():
            ref = tokens_at(h, r, dz)
            return ref, ref, peer
        return ((kind, h, dz % NZ), link, size, refs)

    def y_push(h, dz):
        return [y_copy("yl", h, 0, dz, "l", flip_l), y_copy("yn", h, 0, dz, "n", flip_lh)]

    def y_take(kind, h, dz):
        r = {"yl": 1, "yn": 2, "yr": 3}[kind]
        return ((kind, h, dz % NZ), lambda: tokens_at(h, r, dz))

    def z_first(h, r):
        return [z_push(h, r, d, 1) for d in (1, -1)]

    task(("begin",), body=begin, pushes=x_push("q", 0), work=0.0, prio=-100)
    task(
        ("stats",), deps=[("begin",)], body=statistics, work=1.0, prio=-99,
        pushes=[stats_push(0, partner, "k"), stats_push(1, flip_l, "l"), stats_push(2, flip_lk, "l")]
        + [w_push("q", 0)] + x_push("i", 0),
    )
    task(
        ("bias",), deps=[("stats",)], body=bias_columns, work=0.3, prio=-98,
        pushes=[(("bias", d), "b", 0, lambda d=d: bias_refs(d)) for d in (1, -1, 2)],
    )
    task(
        ("norm",), deps=[("bias",)], body=normalise, work=0.8, prio=-97,
        takes=[(("stats", i), lambda i=i: stats_in.at[i]) for i in range(3)],
        pushes=z_first(0, 0) + z_first(1, 0) + y_push(1, 0) + y_push(0, 0)
        + [w_push("q", 1), w_push("i", 0)],
    )
    gather = []
    for h in range(2):
        for r in range(1 if h == 0 else 4):
            for d in (1, -1):
                for dist in (1, 2, 3):
                    task(
                        ("z", h, r, d, dist), deps=[("norm",)], prio=0 if h == 0 else 5,
                        takes=[z_take(h, r, d, dist)],
                        pushes=[z_push(h, r, d, dist + 1)] + (y_push(0, -d * dist) if h == 0 else []),
                    )
    task(("z4",), takes=[z_take(0, 0, 1, 4), z_take(0, 0, -1, 4)], pushes=y_push(0, 4))
    for dz in range(NZ):
        task(
            ("yl", 0, dz), deps=[("norm",)], prio=1, takes=[y_take("yl", 0, dz)],
            pushes=[y_copy("yr", 0, 1, dz, "n", flip_lh)],
        )
    task(
        ("yl", 1, 0), deps=[("norm",)], prio=1, takes=[y_take("yl", 1, 0)],
        pushes=[y_copy("yr", 1, 1, 0, "n", flip_lh)] + z_first(1, 1),
    )
    task(("yn", 1, 0), deps=[("norm",)], prio=2, takes=[y_take("yn", 1, 0)], pushes=z_first(1, 2))
    task(("yr", 1, 0), deps=[("norm",)], prio=2, takes=[y_take("yr", 1, 0)], pushes=z_first(1, 3))
    task(("w", "i", 1), deps=[("z", 0, 0, 1, 1)], prio=3, pushes=[w_push("i", 1)])
    for w in ("q", "i"):
        task(
            ("w", w), deps=[("norm",)] + ([("w", "i", 1)] if w == "i" else []), prio=2,
            takes=[w_take(w, 0), w_take(w, 1)], pushes=x_push(w, 1),
        )
        x_relay(w, 0, [("norm",)])
        x_relay(w, 1, [("w", w)])
    n = len(CHUNKS)
    for c in range(n):
        pair = (("o", c), ("m", c))
        if c == 0:
            after = [("z", 0, 0, 1, 3), ("z", 0, 0, -1, 3)]
        else:
            after = [("w2s", c - 1)] + ([("w2p", c - 2)] if c >= 2 else [])
        task(("w2s", c), deps=after, prio=6, pushes=[w_push(w) for w in pair])
        if c == 0:
            after = [("x", "i", 0, 1), ("x", "i", 0, -1), ("w", "i"), ("x", "q", 1, 1), ("x", "q", 1, -1)]
        else:
            after = [("w2q", c - 1)] + ([("x", "i", 1, 1), ("x", "i", 1, -1)] if c == 1 else [])
        task(("w2p", c), deps=after, prio=7, pushes=x_push(pair[0], 0) + x_push(pair[1], 0))
        task(
            ("w2q", c), deps=[("w2s", c), ("w2p", c)], prio=7, takes=[w_take(w) for w in pair],
            pushes=x_push(pair[0], 1) + x_push(pair[1], 1),
        )
        for w in pair:
            x_relay(w, 0, [("w2p", c)])
            x_relay(w, 1, [("w2q", c)])
    first_relays = [t.name for t in tasks if t.name[0] in ("z", "z4", "yl", "yn", "yr", "w")]
    first_relays += [("x", w, q, d) for w in ("q", "i") for q in range(2) for d in (1, -1)]

    groups = ((0,), (1, -1), (2, -2), (3, -3), (4,))

    def rows_of(dzs):
        return [pl.ds(pl.multiple_of(zn[dz % NZ] * 128, 128), 128) for dz in dzs]

    def product(lhs, weights, h):
        cols = pl.ds(h * HALF, HALF)
        rhs = weights[..., cols].reshape(384, HALF)
        return lax.dot_general(lhs, rhs, NT, preferred_element_type=F32)

    def project(dzs):
        if dzs == (0,):
            for copy in local_copies[:2]:
                copy.wait()
        rows = rows_of(dzs)
        acc_q = jnp.zeros((128 * len(dzs), 384), F32)
        acc_m = jnp.zeros((128 * len(dzs), 384), F32)
        for h in range(2):
            for q in (yl, nl):
                lhs = jnp.concatenate([xg[h, q, r] for r in rows], axis=0)
                acc_q += product(lhs, WQ.at[q], h)
                if q is yl:
                    acc_m += product(lhs, WM.at[q], h)
        for i, r in enumerate(rows):
            hq[r] = acc_q[i * 128 : (i + 1) * 128]
            hm[r] = acc_m[i * 128 : (i + 1) * 128]

    def project_last(i):
        row = pl.ds(pl.multiple_of(lax.rem(i * 256 + nk * 512, ROWS), 256), 256)
        acc = hm[row]
        for h in range(2):
            acc += product(xg[h, nl, row], WM.at[nl], h)
        hm[row] = acc

    def hq_refs():
        return hq.at[pl.ds(pl.multiple_of(nk * 512, 512), 512)], hxq, partner

    def hm_refs(i):
        theirs = hm.at[pl.ds(pl.multiple_of(nk * 512 + i * 256, 256), 256)]
        return theirs, hxm.at[pl.ds(i * 256, 256)], partner

    k_scale = LINK_RATE / 600e3
    early = x_last("q") + [t for t in x_last("i") if t[0][2] == 0]
    late = [t for t in x_last("i") if t[0][2] == 1]
    early_relays = [("x", w, q, d) for w, q in (("q", 0), ("q", 1), ("i", 0)) for d in (1, -1)]
    late_relays = first_relays
    for g, dzs in enumerate(groups):
        takes, deps = (list(early), list(early_relays)) if g == 0 else ([], [("p", g - 1)])
        for dz in dzs:
            takes += [y_take(kind, 0, dz) for kind in ("yn", "yr")]
            deps += [("yl", 0, dz % NZ)]
            if dz == 0:
                deps += [("norm",), ("yl", 1, 0), ("yn", 1, 0), ("yr", 1, 0)]
            elif dz == 4:
                deps += [("z4",)]
                takes += [z_take(1, r, d, 4) for r in range(4) for d in (1, -1)]
            else:
                d = -1 if dz > 0 else 1
                deps += [("z", 0, 0, d, abs(dz))] + [("z", 1, r, d, abs(dz)) for r in range(4)]
        task(
            ("p", g), takes=takes, deps=deps, body=lambda dzs=dzs: project(dzs), prio=30,
            work=0.9 if len(dzs) == 1 else 1.4,
            pushes=[(("hq",), "k", 512 * 384 * 4 * k_scale, hq_refs)] if g == 4 else [],
        )
    for i in range(4):
        task(
            ("pl", i), takes=late if i == 0 else [],
            deps=late_relays + [("p", 4)] if i == 0 else [("pl", i - 1)],
            body=lambda i=i: project_last(i), work=0.5, prio=10,
            pushes=[(("hm", i), "k", 256 * 384 * 4 * k_scale, lambda i=i: hm_refs(i))] if i < 2 else [],
        )

    def head_norm(values, gain):
        centred = values - jnp.mean(values, -1, keepdims=True)
        spread = jnp.mean(centred * centred, -1, keepdims=True)
        return (centred * lax.rsqrt(spread + EPS) * gain[...].astype(F32)).astype(BF16)

    def own_rows(i):
        return pl.ds(pl.multiple_of(k * 512 + i * IMAGE, IMAGE), IMAGE)

    def attend(i):
        mine = pl.ds(i * IMAGE, IMAGE)
        joined = hq[own_rows(i)] + hxq[mine]
        q = head_norm(joined[:, 0:128], q_gain)
        kk = head_norm(joined[:, 128:256], k_gain)
        v = joined[:, 256:384].astype(BF16)
        scores = lax.dot_general(q, kk, NT, preferred_element_type=F32) * HD ** (-0.5)
        e = jnp.exp(scores - jnp.max(scores, -1, keepdims=True))
        probs = (e / jnp.sum(e, -1, keepdims=True)).astype(BF16)
        attended = jnp.dot(probs, v, preferred_element_type=F32)
        att[k, mine, pl.ds(0, 128)] = attended.astype(BF16)

    def activate(i):
        mine = pl.ds(i * IMAGE, IMAGE)
        unit = (lax.broadcasted_iota(jnp.int32, (IMAGE, 128), 1) == 0).astype(F32).astype(BF16)
        pre = hm[own_rows(i)] + hxm[mine] + lax.dot_general(
            unit, BI[...].reshape(384, 128), NT, preferred_element_type=F32
        )
        hidden = 0.5 * pre * (1.0 + lax.erf(pre * (0.5 ** 0.5)))
        att[k, mine, pl.ds(128, 384)] = hidden.astype(BF16)

    def att_refs(i):
        ref = att.at[k, pl.ds(i * IMAGE, IMAGE)]
        return ref, ref, partner

    for i in range(2):
        task(
            ("attend", i), deps=[("pl", 3)] + [("attend", 0)] * i, prio=10, work=0.45,
            takes=[(("hq",), lambda: hxq)] if i == 0 else [], body=lambda i=i: attend(i),
        )
    for i in range(2):
        takes = [(("hm", i), lambda i=i: hxm.at[pl.ds(i * 256, 256)])]
        if i == 0:
            takes += [(("bias", d), lambda d=d: BI.at[xs[-d % NX]]) for d in (1, -1, 2)]
        task(
            ("image", i), takes=takes, deps=[("attend", 1)] + [("image", 0)] * i, prio=10, work=0.45,
            body=lambda i=i: activate(i),
            pushes=[(("att", i), "k", 256 * 512 * 2 * k_scale, lambda i=i: att_refs(i))],
        )

    def output_terms(c, half):
        if c == 0 and half == 0:
            for copy in local_copies[2:]:
                copy.wait()
        _, c0, width = CHUNKS[c]
        who = k if half == 0 else nk
        cols = slice(c0, c0 + width)
        for i in range(2):
            row = pl.multiple_of(who * 512 + i * 256, 256)
            a = att[who, pl.ds(i * 256, 256)]
            for q in range(2):
                part[q, pl.ds(row, 256), pl.ds(c0, width)] = jnp.dot(
                    a[:, :128], OW[q, :, :, cols].reshape(128, width), preferred_element_type=F32
                ) + jnp.dot(
                    a[:, 128:], MO[q, :, :, cols].reshape(384, width), preferred_element_type=F32
                )

    for c, (_, _, width) in enumerate(CHUNKS):
        pair = (("o", c), ("m", c))
        for half in range(2):
            deps = [("image", 1)]
            deps += [("x", w, q, d) for w in pair for q in range(2) for d in (1, -1)]
            deps += [("terms", c, 0)] if half else []
            deps += [("terms", c - 1, 1)] if c else []
            takes = (x_last(pair[0]) + x_last(pair[1])) if half == 0 else []
            if c == 0 and half == 1:
                takes = [
                    (("att", i), lambda i=i: att.at[nk, pl.ds(i * IMAGE, IMAGE)]) for i in range(2)
                ]
            task(
                ("terms", c, half), takes=takes, deps=deps, prio=9, work=1.44 * width / 768,
                body=lambda c=c, half=half: output_terms(c, half),
            )

    half = BLOCK // 2

    def term(c, r, dz):
        row = pl.multiple_of((zn[dz % NZ] * 2 + rel_h[r]) * BLOCK, BLOCK)
        return part.at[rel_l[r], pl.ds(row, BLOCK), pl.ds(*CHUNKS[c][1:])]

    def reduction(c):
        kind, _, width = CHUNKS[c]
        zs, zr, ns, nr, ms, mr = chunk_refs[6 * c : 6 * c + 6]
        block, groups = BLOCK * width * 2, (1 if kind == "y" else 4)
        work = 0.05 + 0.12 * width / HALF
        ready = ("terms", c, 1)

        def along_z(g, r, d, dist):
            slot, landing = zs.at[g, 0 if d == 1 else 1, dist - 1], zr.at[g, 0 if d == 1 else 1, dist - 1]
            if dist == 4:
                slot, landing = slot.at[pl.ds(0, half)], landing.at[pl.ds(0, half)]
            before = zr.at[g, 0 if d == 1 else 1, min(dist, 3)]
            if dist == 3:
                before = before.at[pl.ds(0, half)]
            lo = 0 if d == 1 else half

            def body():
                blk = term(c, r, d * dist)
                if dist == 4:
                    slot[...] = blk[pl.ds(lo, half)].astype(BF16)
                elif dist == 3:
                    slot[pl.ds(half - lo, half)] = blk[pl.ds(half - lo, half)].astype(BF16)
                    slot[pl.ds(lo, half)] = (
                        blk[pl.ds(lo, half)] + before[...].astype(F32)
                    ).astype(BF16)
                else:
                    slot[...] = (blk[...] + before[...].astype(F32)).astype(BF16)

            from_y = ("y_end", c, (d * dist) % NZ) if kind == "y" else ready
            prio = 3 if kind == "y" else 8 - dist * 0.5 + (0 if r in (2, 3) else 0.3)
            task(
                ("c", c, r, d, dist), body=body, work=work, prio=prio + c * 0.01,
                takes=[] if dist == 4 else [(("c", c, r, d, dist + 1), lambda: before)],
                deps=[from_y] + ([] if dist == 4 else [("c", c, r, d, dist + 1)]),
                pushes=[
                    (("c", c, r, d, dist), ("z", d), block // 2 if dist == 4 else block,
                     lambda: (slot, landing, at_z(d)))
                ],
            )

        def z_end(g, r):
            def body():
                blk = term(c, r, 0)
                blk[...] = blk[...] + zr[g, 0, 0].astype(F32) + zr[g, 1, 0].astype(F32)
            task(
                ("z_end", c, r), body=body, work=work, prio=2,
                takes=[(("c", c, r, d, 1), lambda i=i: zr.at[g, i, 0]) for i, d in enumerate((1, -1))],
                deps=[("c", c, r, d, 1) for d in (1, -1)] + ([("y_end", c, 0)] if kind == "y" else []),
            )

        def along_y(g, dz, deps_out, deps_mid, deps_end, prios):
            tree = (c + dz) % 2
            far, near = ((flip_lh, "n"), (flip_l, "l")) if tree == 0 else ((flip_l, "l"), (flip_lh, "n"))
            direct, mid = (2, 1) if tree == 0 else (1, 2)

            def out_body():
                for j, r in enumerate((direct, 3)):
                    ns[g, j] = term(c, r, dz)[...].astype(BF16)

            def mid_body():
                ms[g] = (term(c, mid, dz)[...] + nr[g, 1].astype(F32)).astype(BF16)

            def end_body():
                blk = term(c, 0, dz)
                blk[...] = blk[...] + nr[g, 0].astype(F32) + mr[g].astype(F32)

            task(
                ("y_out", c, dz), body=out_body, deps=deps_out(direct), prio=prios[0],
                work=0.05 + 0.15 * width / HALF,
                pushes=[
                    (("n", c, dz, j), far[1], block, lambda j=j: (ns.at[g, j], nr.at[g, j], far[0]))
                    for j in (1, 0)
                ],
            )
            task(
                ("y_mid", c, dz), body=mid_body, work=work, prio=prios[1],
                takes=[(("n", c, dz, 1), lambda: nr.at[g, 1])],
                deps=[("y_out", c, dz)] + deps_mid(mid),
                pushes=[(("m", c, dz), near[1], block, lambda: (ms.at[g], mr.at[g], near[0]))],
            )
            task(
                ("y_end", c, dz), body=end_body, work=work, prio=prios[2],
                takes=[(("n", c, dz, 0), lambda: nr.at[g, 0]), (("m", c, dz), lambda: mr.at[g])],
                deps=[("y_mid", c, dz)] + deps_end,
            )

        if kind == "y":
            for dz in range(NZ):
                far = min(dz, NZ - dz)
                along_y(
                    dz, dz, lambda r: [ready], lambda r: [], [],
                    (20 - far, 4 - far * 0.1, 5 - far * 0.1),
                )
        for g in range(groups):
            for d in (1, -1):
                for dist in (4, 3, 2, 1):
                    along_z(g, g, d, dist)
            z_end(g, g)
        if kind == "z":
            along_y(
                0, 0, lambda r: [("z_end", c, r), ("z_end", c, 3)], lambda r: [("z_end", c, r)],
                [("z_end", c, 0)], (1, 1, 1),
            )

    for c in range(n):
        reduction(c)

    for step in in_order(tasks):
        for key, ref in step.takes:
            take(key, ref())
        if step.body is not None:
            step.body()
        for key, _, _, refs in step.pushes:
            push(key, *refs())

    own = pl.ds(pl.multiple_of((z * 2 + yh) * BLOCK, BLOCK), BLOCK)
    out[...] = part[yl, own]
    for copy in started:
        copy.wait_send()
    assert len(index) <= N_SEMS, len(index)


def per_device(
    tokens, ln_gain, qkv_weight, q_gain, k_gain, out_weight, mlp_in, mlp_bias, mlp_out, out_bias
):
    wq = jnp.transpose(qkv_weight, (1, 2, 3, 0))
    wm = jnp.transpose(mlp_in).reshape(2, UNITS, PIECE)
    mo = mlp_out.reshape(2, UNITS, PIECE)
    bias = jnp.pad(mlp_bias, (0, 64)).reshape(2, 128)
    vm, hbm = pl.BlockSpec(memory_space=pltpu.VMEM), pl.BlockSpec(memory_space=pl.ANY)
    scratch = [
        pltpu.VMEM((BLOCK, PIECE), BF16),
        pltpu.VMEM((8, 128), F32),
        pltpu.VMEM((3, 8, 128), F32),
        pltpu.VMEM((2, 2, ROWS, HALF), BF16),
        pltpu.VMEM((2, 3, NX, 32, PIECE), BF16),
        pltpu.VMEM((2, NX, UNITS, PIECE), BF16),
        pltpu.VMEM((256, 128), BF16),
        pltpu.VMEM((NX, UNITS, 128), BF16),
        pltpu.VMEM((2, NX, 32, PIECE), BF16),
        pltpu.VMEM((2, NX, UNITS, PIECE), BF16),
        pltpu.VMEM((ROWS, 384), F32),
        pltpu.VMEM((ROWS, 384), F32),
        pltpu.VMEM((512, 384), F32),
        pltpu.VMEM((512, 384), F32),
        pltpu.VMEM((2, 512, 512), BF16),
        pltpu.VMEM((2, ROWS, PIECE), F32),
    ]
    for kind, _, width in CHUNKS:
        block = (BLOCK, width)
        groups, ys = (1, NZ) if kind == "y" else (4, 1)
        scratch += [pltpu.VMEM((groups, 2, 4, *block), BF16)] * 2
        scratch += [pltpu.VMEM((ys, 2, *block), BF16)] * 2
        scratch += [pltpu.VMEM((ys, *block), BF16)] * 2
    scratch += [
        pltpu.SemaphoreType.DMA((N_SEMS,)),
        pltpu.SemaphoreType.DMA((N_SEMS,)),
        pltpu.SemaphoreType.DMA((5,)),
    ]
    sums = pl.pallas_call(
        kernel,
        out_shape=jax.ShapeDtypeStruct((BLOCK, PIECE), F32),
        in_specs=[hbm, vm, hbm, hbm, vm, vm, hbm, vm, hbm],
        out_specs=vm,
        scratch_shapes=scratch,
        compiler_params=pltpu.CompilerParams(
            collective_id=0, has_side_effects=True, vmem_limit_bytes=60 * 1024 * 1024
        ),
        name="layer",
    )(
        tokens, ln_gain.reshape(PIECE // 128, 128), wq, wm, q_gain.reshape(1, HD),
        k_gain.reshape(1, HD), out_weight, bias, mo,
    )
    return tokens.astype(F32) + sums + out_bias.astype(F32)


def solution(mesh):
    split = Mesh(
        mesh.devices.reshape(NX, 2, 2, NZ, 2), ("x", "yl", "k", "z", "yh")
    )
    token_axes, row, col = ("x", "z", "yh"), ("yl", "k"), ("z", "yh")
    placed = (
        P(token_axes, row),
        P(row),
        P(row, None, col, "x"),
        P(),
        P(),
        P(col, "x", row),
        P(row, token_axes),
        P(token_axes),
        P(token_axes, row),
        P(row),
    )
    return jax.shard_map(
        per_device, mesh=split, in_specs=placed, out_specs=P(token_axes, row), check_vma=False
    )
```

```python
import jax
import jax.numpy as jnp
from jax import lax
from jax.experimental import pallas as pl
from jax.experimental.pallas import tpu as pltpu
from jax.sharding import Mesh
from jax.sharding import PartitionSpec as P

D = 6144
HD = 128
IMAGE = 256
NX, NZ = 4, 8
BLOCK = 64
ROWS = 1024
PIECE = 1536
HALF = 768
UNITS = 96
EPS = 1e-06
MESH = pl.DeviceIdType.MESH
F32, BF16 = jnp.float32, jnp.bfloat16
NT = (((1,), (1,)), ((), ()))


CHUNKS = (("y", 0, 256), ("z", 256, 256), ("y", 512, 512), ("z", 1024, 256), ("y", 1280, 256))
N_SEMS = 360
LAGS = ((2, (0, 1)),)
LINK_RATE, LATENCY, ISSUE = 44e3, 2.3, 0.03

ORDER = (
    0, 1, 2, 58, 3, 46, 4, 57, 69, 7, 43, 35, 44, 47, 68, 8, 60, 13, 5, 10, 19, 45, 52, 53, 16, 49, 9, 6, 54, 11,
    22, 48, 50, 42, 20, 36, 51, 28, 31, 25, 37, 12, 71, 59, 75, 14, 41, 72, 34, 79, 17, 56, 61, 90, 29, 38, 32, 26,
    70, 40, 55, 80, 23, 64, 18, 21, 39, 15, 112, 33, 30, 65, 67, 27, 24, 113, 114, 115, 116, 63, 117, 81, 74, 78,
    66, 62, 91, 118, 73, 76, 77, 101, 119, 83, 92, 120, 121, 122, 123, 124, 89, 82, 86, 85, 84, 125, 87, 88, 126,
    144, 94, 141, 150, 98, 147, 138, 127, 93, 96, 135, 156, 128, 99, 186, 168, 172, 195, 177, 190, 153, 97, 100,
    95, 181, 145, 199, 142, 102, 103, 129, 151, 148, 130, 219, 216, 187, 210, 196, 225, 182, 131, 132, 200, 104,
    262, 108, 267, 258, 169, 213, 271, 240, 244, 253, 249, 143, 173, 191, 105, 157, 110, 152, 178, 109, 111, 149,
    222, 197, 107, 106, 163, 183, 146, 220, 268, 259, 272, 263, 250, 241, 245, 133, 254, 134, 174, 291, 201, 159,
    269, 154, 164, 184, 198, 217, 260, 297, 288, 179, 264, 223, 294, 273, 188, 158, 192, 221, 292, 160, 231, 214,
    235, 255, 289, 251, 170, 228, 285, 202, 265, 155, 261, 218, 295, 226, 279, 270, 246, 293, 180, 303, 307, 211,
    274, 224, 236, 232, 139, 252, 298, 193, 286, 229, 189, 215, 207, 290, 282, 296, 242, 256, 300, 308, 175, 165,
    304, 203, 275, 185, 233, 227, 204, 212, 237, 299, 171, 257, 161, 247, 287, 283, 276, 194, 136, 305, 230, 309,
    301, 243, 266, 234, 208, 166, 238, 205, 140, 280, 284, 162, 306, 176, 277, 302, 310, 248, 206, 137, 167, 209,
    239, 278, 281, 311,
)


class Task:
    def __init__(self, name, takes=(), deps=(), work=0.02, body=None, pushes=(), prio=0.0):
        self.name, self.takes, self.deps, self.work = name, list(takes), list(deps), work
        self.body, self.pushes, self.prio = body, list(pushes), prio


def in_order(tasks):
    now, arrival, free, done, order, left = 0.0, {}, {}, set(), [], list(tasks)
    while left:
        best = None
        for task in left:
            if all(d in done for d in task.deps) and all(k in arrival for k, _ in task.takes):
                ready = max([now] + [arrival[k] for k, _ in task.takes])
                if best is None or (ready, task.prio) < best[:2]:
                    best = (ready, task.prio, task)
        now, _, task = best
        now += task.work
        for key, link, size, _ in task.pushes:
            now += ISSUE
            free[link] = max(now, free.get(link, 0.0)) + size / LINK_RATE
            arrival[key] = free[link] + LATENCY
        done.add(task.name)
        order.append(task)
        left.remove(task)
    return order


def kernel(
    tok_hbm, ln_gain, wq, wm, q_gain, k_gain, ow, bias_in, mo, out_bias,
    out,
    tok, stats, stats_in, xg, WQ, WM, BV, BI, OW, MO, hq, hm, hxq, hxm, att, part, *rest,
):
    chunk_refs, (send, recv, local) = rest[:-3], rest[-3:]
    x, yl, k = lax.axis_index("x"), lax.axis_index("yl"), lax.axis_index("k")
    z, yh = lax.axis_index("z"), lax.axis_index("yh")
    nl, nk, nh = 1 - yl, 1 - k, 1 - yh
    xs = [lax.rem(x + d, NX) for d in range(NX)]
    zn = [lax.rem(z + d, NZ) for d in range(NZ)]
    at_x = lambda d: {"x": xs[d % NX]}
    at_z = lambda d: {"z": zn[d % NZ]}
    flip_l, flip_lh = {"yl": nl}, {"yl": nl, "yh": nh}
    partner, flip_lk = {"k": nk}, {"yl": nl, "k": nk}
    rel_l, rel_h = (yl, nl, nl, yl), (yh, yh, nh, nh)

    index, started = {}, []

    def push(key, src, dst, peer):
        i = index.setdefault(key, len(index))
        copy = pltpu.make_async_remote_copy(
            src_ref=src, dst_ref=dst, send_sem=send.at[i], recv_sem=recv.at[i],
            device_id=peer, device_id_type=MESH,
        )
        copy.start()
        started.append(copy)

    def take(key, dst):
        i = index.setdefault(key, len(index))
        pltpu.make_async_remote_copy(
            src_ref=dst, dst_ref=dst, send_sem=send.at[i], recv_sem=recv.at[i],
            device_id=partner, device_id_type=MESH,
        ).wait_recv()

    tok_copy = pltpu.make_async_copy(tok_hbm, tok, local.at[4])
    tok_copy.start()
    barrier = pltpu.get_barrier_semaphore()
    peers = [at_x(1), at_x(-1), at_x(2), at_z(1), at_z(-1), flip_l, flip_lh, partner, flip_lk]
    for peer in peers:
        pl.semaphore_signal(barrier, inc=1, device_id=peer, device_id_type=MESH)

    tasks = []

    def task(*args, **kwargs):
        tasks.append(Task(*args, **kwargs))

    def cols_of(w):
        return pl.ds(*CHUNKS[w[1]][1:]) if isinstance(w, tuple) else pl.ds(0, PIECE)

    def stored(w, j, c=None):
        c = cols_of(w) if c is None else c
        if w == "q":
            return wq.at[:, j, :, c]
        return {"i": wm, "o": ow, "m": mo}[w[0]].at[j, :, c]

    def gathered(w, q, s, c=None):
        c = cols_of(w) if c is None else c
        if w == "q":
            return WQ.at[q, :, s, :, c]
        return {"i": WM, "o": OW, "m": MO}[w[0]].at[q, s, :, c]

    def part_of(w, q, s, d):
        lo = 0 if d == 1 else 1
        if w in ("q", "i"):
            return gathered(w, q, s, pl.ds(lo * HALF, HALF))
        rows = 16 if w[0] == "o" else 48
        ref = OW if w[0] == "o" else MO
        return ref.at[q, s, pl.ds(lo * rows, rows), cols_of(w)]

    def bytes_of(w):
        width = CHUNKS[w[1]][2] if isinstance(w, tuple) else PIECE
        return (32 if w[0] == "o" else UNITS) * width * 2

    quarter = (yl, nl)

    def x_push(w, q):
        def refs(d):
            dst = gathered(w, quarter[q], x)
            return (stored(w, yl) if q == 0 else dst), dst, at_x(d)
        return [(("x", w, q, d), ("x", d), bytes_of(w), lambda d=d: refs(d)) for d in (1, -1)]

    def w_push(w, h=None):
        c = None if h is None else pl.ds(h * HALF, HALF)
        size = bytes_of(w) if h is None else bytes_of(w) // 2
        return (("w", w, h), "l", size, lambda: (stored(w, nl, c), gathered(w, yl, x, c), flip_l))

    def w_take(w, h=None):
        c = None if h is None else pl.ds(h * HALF, HALF)
        return (("w", w, h), lambda: gathered(w, nl, x, c))

    def x_relay(w, q, deps):
        for d in (1, -1):
            def refs(d=d):
                ref = part_of(w, quarter[q], xs[-d % NX], d)
                return ref, ref, at_x(d)
            task(
                ("x", w, q, d), deps=deps, prio=-1,
                takes=[(("x", w, q, d), lambda d=d: gathered(w, quarter[q], xs[-d % NX]))],
                pushes=[(("x2", w, q, d), ("x", d), bytes_of(w) // 2, refs)],
            )

    def x_last(w):
        return [
            (("x2", w, q, d), lambda q=q, d=d: part_of(w, quarter[q], xs[2], d))
            for q in range(2) for d in (1, -1)
        ]

    def stats_push(i, peer, link):
        return (("stats", i), link, 8 * 128 * 4, lambda: (stats, stats_in.at[i], peer))

    local_copies = []

    def begin():
        pl.semaphore_wait(barrier, len(peers))
        for i, w in enumerate(("q", "i")):
            copy = pltpu.make_async_copy(stored(w, yl), gathered(w, yl, x), local.at[i])
            copy.start()
            local_copies.append(copy)
        for i, (src, dst) in enumerate(((ow, OW), (mo, MO))):
            copy = pltpu.make_async_copy(src.at[yl], dst.at[yl, x], local.at[2 + i])
            copy.start()
            local_copies.append(copy)

    def statistics():
        tok_copy.wait()
        t = tok[...].astype(F32)
        s1 = jnp.sum(t, 1, keepdims=True)
        s2 = jnp.sum(t * t, 1, keepdims=True)
        lane = lax.broadcasted_iota(jnp.int32, (BLOCK, 128), 1)
        both = jnp.where(lane < 64, s1, s2)
        turned = jnp.concatenate([both, both], axis=0).T
        row = lax.broadcasted_iota(jnp.int32, (8, 128), 0)
        stats[...] = jnp.where(row < 4, turned[0:1], turned[64:65])

    def bias_columns():
        for i, count in enumerate((128, 64)):
            b = bias_in[pl.ds(i * 128, count)].astype(F32).reshape(1, count)
            if count < 128:
                b = jnp.concatenate([b, b], axis=1)
            BV[pl.ds(i * 128, 128), :] = jnp.broadcast_to(b, (128, 128)).T.astype(BF16)
        mine = pl.ds(pl.multiple_of(yl * UNITS, 32), UNITS)
        BI[x] = BV[mine, :]

    def bias_refs(d):
        return BI.at[x], BI.at[x], at_x(d)

    def normalise():
        total = stats[...] + stats_in[0] + stats_in[1] + stats_in[2]
        mean = total[0:1] * (1.0 / D)
        var = total[4:5] * (1.0 / D) - mean * mean
        row = lax.broadcasted_iota(jnp.int32, (128, 128), 0)
        turned = jnp.where(row < 64, mean, lax.rsqrt(var + EPS)).T
        mean, scale = turned[:BLOCK, 0:1], turned[:BLOCK, 64:65]
        t = tok[...].astype(F32)
        g = ln_gain[...].astype(F32)
        g = jnp.concatenate([g[i : i + 1] for i in range(PIECE // 128)], axis=1)
        normed = ((t - mean) * scale * g).astype(BF16)
        own_row = pl.multiple_of((z * 2 + yh) * BLOCK, BLOCK)
        xg[0, yl, pl.ds(own_row, BLOCK)] = normed[:, :HALF]
        xg[1, yl, pl.ds(own_row, BLOCK)] = normed[:, HALF:]

    size = BLOCK * HALF * 2

    def tokens_at(h, r, dz):
        row = pl.multiple_of((zn[dz % NZ] * 2 + rel_h[r]) * BLOCK, BLOCK)
        return xg.at[h, rel_l[r], pl.ds(row, BLOCK)]

    def z_half(ref, d):
        return ref.at[pl.ds(0 if d == 1 else BLOCK // 2, BLOCK // 2)]

    def z_ref(h, r, d, dist, back):
        ref = tokens_at(h, r, -d * (dist - back))
        return z_half(ref, d) if dist == 4 else ref

    def z_push(h, r, d, dist):
        def refs():
            ref = z_ref(h, r, d, dist, 1)
            return ref, ref, at_z(d)
        return (("z", h, r, d, dist), ("z", d), size // 2 if dist == 4 else size, refs)

    def z_take(h, r, d, dist):
        return (("z", h, r, d, dist), lambda: z_ref(h, r, d, dist, 0))

    def y_copy(kind, h, r, dz, link, peer):
        def refs():
            ref = tokens_at(h, r, dz)
            return ref, ref, peer
        return ((kind, h, dz % NZ), link, size, refs)

    def y_push(h, dz):
        return [y_copy("yl", h, 0, dz, "l", flip_l), y_copy("yn", h, 0, dz, "n", flip_lh)]

    def y_take(kind, h, dz):
        r = {"yl": 1, "yn": 2, "yr": 3}[kind]
        return ((kind, h, dz % NZ), lambda: tokens_at(h, r, dz))

    def z_first(h, r):
        return [z_push(h, r, d, 1) for d in (1, -1)]

    task(("begin",), body=begin, pushes=x_push("q", 0), work=0.0, prio=-100)
    task(
        ("stats",), deps=[("begin",)], body=statistics, work=1.0, prio=-99,
        pushes=[stats_push(0, partner, "k"), stats_push(1, flip_l, "l"), stats_push(2, flip_lk, "l")]
        + [w_push("q", 0)] + x_push("i", 0),
    )
    task(
        ("bias",), deps=[("stats",)], body=bias_columns, work=0.3, prio=-98,
        pushes=[(("bias", d), "b", 0, lambda d=d: bias_refs(d)) for d in (1, -1, 2)],
    )
    task(
        ("norm",), deps=[("bias",)], body=normalise, work=0.8, prio=-97,
        takes=[(("stats", i), lambda i=i: stats_in.at[i]) for i in range(3)],
        pushes=z_first(0, 0) + z_first(1, 0) + y_push(1, 0) + y_push(0, 0)
        + [w_push("q", 1), w_push("i", 0)],
    )
    gather = []
    for h in range(2):
        for r in range(1 if h == 0 else 4):
            for d in (1, -1):
                for dist in (1, 2, 3):
                    task(
                        ("z", h, r, d, dist), deps=[("norm",)], prio=0 if h == 0 else 5,
                        takes=[z_take(h, r, d, dist)],
                        pushes=[z_push(h, r, d, dist + 1)] + (y_push(0, -d * dist) if h == 0 else []),
                    )
    task(("z4",), takes=[z_take(0, 0, 1, 4), z_take(0, 0, -1, 4)], pushes=y_push(0, 4))
    for dz in range(NZ):
        task(
            ("yl", 0, dz), deps=[("norm",)], prio=1, takes=[y_take("yl", 0, dz)],
            pushes=[y_copy("yr", 0, 1, dz, "n", flip_lh)],
        )
    task(
        ("yl", 1, 0), deps=[("norm",)], prio=1, takes=[y_take("yl", 1, 0)],
        pushes=[y_copy("yr", 1, 1, 0, "n", flip_lh)] + z_first(1, 1),
    )
    task(("yn", 1, 0), deps=[("norm",)], prio=2, takes=[y_take("yn", 1, 0)], pushes=z_first(1, 2))
    task(("yr", 1, 0), deps=[("norm",)], prio=2, takes=[y_take("yr", 1, 0)], pushes=z_first(1, 3))
    task(("w", "i", 1), deps=[("z", 0, 0, 1, 1)], prio=3, pushes=[w_push("i", 1)])
    for w in ("q", "i"):
        task(
            ("w", w), deps=[("norm",)] + ([("w", "i", 1)] if w == "i" else []), prio=2,
            takes=[w_take(w, 0), w_take(w, 1)], pushes=x_push(w, 1),
        )
        x_relay(w, 0, [("norm",)])
        x_relay(w, 1, [("w", w)])
    n = len(CHUNKS)
    for c in range(n):
        pair = (("o", c), ("m", c))
        if c == 0:
            after = [("z", 0, 0, 1, 3), ("z", 0, 0, -1, 3)]
        else:
            after = [("w2s", c - 1)] + ([("w2p", c - 2)] if c >= 2 else [])
        task(("w2s", c), deps=after, prio=6, pushes=[w_push(w) for w in pair])
        if c == 0:
            after = [("x", "i", 0, 1), ("x", "i", 0, -1), ("w", "i"), ("x", "q", 1, 1), ("x", "q", 1, -1)]
        else:
            after = [("w2q", c - 1)] + ([("x", "i", 1, 1), ("x", "i", 1, -1)] if c == 1 else [])
            for lag, qs in LAGS:
                if c >= lag:
                    after += [("x", (w, c - lag), q, d) for w in "om" for q in qs for d in (1, -1)]
        task(("w2p", c), deps=after, prio=7, pushes=x_push(pair[0], 0) + x_push(pair[1], 0))
        task(
            ("w2q", c), deps=[("w2s", c), ("w2p", c)], prio=7, takes=[w_take(w) for w in pair],
            pushes=x_push(pair[0], 1) + x_push(pair[1], 1),
        )
        for w in pair:
            x_relay(w, 0, [("w2p", c)])
            x_relay(w, 1, [("w2q", c)])
    first_relays = [t.name for t in tasks if t.name[0] in ("z", "z4", "yl", "yn", "yr", "w")]
    first_relays += [("x", w, q, d) for w in ("q", "i") for q in range(2) for d in (1, -1)]

    groups = ((0,), (1, -1), (2, -2), (3, -3), (4,))

    def rows_of(dzs):
        return [pl.ds(pl.multiple_of(zn[dz % NZ] * 128, 128), 128) for dz in dzs]

    def product(lhs, weights, h):
        cols = pl.ds(h * HALF, HALF)
        rhs = weights[..., cols].reshape(384, HALF)
        return lax.dot_general(lhs, rhs, NT, preferred_element_type=F32)

    def project(dzs):
        if dzs == (0,):
            for copy in local_copies[:2]:
                copy.wait()
        rows = rows_of(dzs)
        acc_q = jnp.zeros((128 * len(dzs), 384), F32)
        acc_m = jnp.zeros((128 * len(dzs), 384), F32)
        for h in range(2):
            for q in (yl, nl):
                lhs = jnp.concatenate([xg[h, q, r] for r in rows], axis=0)
                acc_q += product(lhs, WQ.at[q], h)
                if q is yl:
                    acc_m += product(lhs, WM.at[q], h)
        for i, r in enumerate(rows):
            hq[r] = acc_q[i * 128 : (i + 1) * 128]
            hm[r] = acc_m[i * 128 : (i + 1) * 128]

    def project_last(i):
        row = pl.ds(pl.multiple_of(lax.rem(i * 256 + nk * 512, ROWS), 256), 256)
        acc = hm[row]
        for h in range(2):
            acc += product(xg[h, nl, row], WM.at[nl], h)
        hm[row] = acc

    def hq_refs():
        return hq.at[pl.ds(pl.multiple_of(nk * 512, 512), 512)], hxq, partner

    def hm_refs(i):
        theirs = hm.at[pl.ds(pl.multiple_of(nk * 512 + i * 256, 256), 256)]
        return theirs, hxm.at[pl.ds(i * 256, 256)], partner

    k_scale = LINK_RATE / 600e3
    early = x_last("q") + [t for t in x_last("i") if t[0][2] == 0]
    late = [t for t in x_last("i") if t[0][2] == 1]
    early_relays = [("x", w, q, d) for w, q in (("q", 0), ("q", 1), ("i", 0)) for d in (1, -1)]
    late_relays = first_relays
    for g, dzs in enumerate(groups):
        takes, deps = (list(early), list(early_relays)) if g == 0 else ([], [("p", g - 1)])
        for dz in dzs:
            takes += [y_take(kind, 0, dz) for kind in ("yn", "yr")]
            deps += [("yl", 0, dz % NZ)]
            if dz == 0:
                deps += [("norm",), ("yl", 1, 0), ("yn", 1, 0), ("yr", 1, 0)]
            elif dz == 4:
                deps += [("z4",)]
                takes += [z_take(1, r, d, 4) for r in range(4) for d in (1, -1)]
            else:
                d = -1 if dz > 0 else 1
                deps += [("z", 0, 0, d, abs(dz))] + [("z", 1, r, d, abs(dz)) for r in range(4)]
        task(
            ("p", g), takes=takes, deps=deps, body=lambda dzs=dzs: project(dzs), prio=30,
            work=0.9 if len(dzs) == 1 else 1.4,
            pushes=[(("hq",), "k", 512 * 384 * 4 * k_scale, hq_refs)] if g == 4 else [],
        )
    for i in range(4):
        task(
            ("pl", i), takes=late if i == 0 else [],
            deps=late_relays + [("p", 4)] if i == 0 else [("pl", i - 1)],
            body=lambda i=i: project_last(i), work=0.5, prio=10,
            pushes=[(("hm", i), "k", 256 * 384 * 4 * k_scale, lambda i=i: hm_refs(i))] if i < 2 else [],
        )

    def head_norm(values, gain):
        centred = values - jnp.mean(values, -1, keepdims=True)
        spread = jnp.mean(centred * centred, -1, keepdims=True)
        return (centred * lax.rsqrt(spread + EPS) * gain[...].astype(F32)).astype(BF16)

    def own_rows(i):
        return pl.ds(pl.multiple_of(k * 512 + i * IMAGE, IMAGE), IMAGE)

    def attend(i):
        mine = pl.ds(i * IMAGE, IMAGE)
        joined = hq[own_rows(i)] + hxq[mine]
        q = head_norm(joined[:, 0:128], q_gain)
        kk = head_norm(joined[:, 128:256], k_gain)
        v = joined[:, 256:384].astype(BF16)
        scores = lax.dot_general(q, kk, NT, preferred_element_type=F32) * HD ** (-0.5)
        e = jnp.exp(scores - jnp.max(scores, -1, keepdims=True))
        probs = (e / jnp.sum(e, -1, keepdims=True)).astype(BF16)
        attended = jnp.dot(probs, v, preferred_element_type=F32)
        att[k, mine, pl.ds(0, 128)] = attended.astype(BF16)

    def activate(i):
        mine = pl.ds(i * IMAGE, IMAGE)
        unit = (lax.broadcasted_iota(jnp.int32, (IMAGE, 128), 1) == 0).astype(F32).astype(BF16)
        pre = hm[own_rows(i)] + hxm[mine] + lax.dot_general(
            unit, BI[...].reshape(384, 128), NT, preferred_element_type=F32
        )
        hidden = 0.5 * pre * (1.0 + lax.erf(pre * (0.5 ** 0.5)))
        att[k, mine, pl.ds(128, 384)] = hidden.astype(BF16)

    def att_refs(i):
        ref = att.at[k, pl.ds(i * IMAGE, IMAGE)]
        return ref, ref, partner

    for i in range(2):
        task(
            ("attend", i), deps=[("pl", 3)] + [("attend", 0)] * i, prio=10, work=0.45,
            takes=[(("hq",), lambda: hxq)] if i == 0 else [], body=lambda i=i: attend(i),
        )
    for i in range(2):
        takes = [(("hm", i), lambda i=i: hxm.at[pl.ds(i * 256, 256)])]
        if i == 0:
            takes += [(("bias", d), lambda d=d: BI.at[xs[-d % NX]]) for d in (1, -1, 2)]
        task(
            ("image", i), takes=takes, deps=[("attend", 1)] + [("image", 0)] * i, prio=10, work=0.45,
            body=lambda i=i: activate(i),
            pushes=[(("att", i), "k", 256 * 512 * 2 * k_scale, lambda i=i: att_refs(i))],
        )

    def output_terms(c, half):
        if c == 0 and half == 0:
            for copy in local_copies[2:]:
                copy.wait()
        _, c0, width = CHUNKS[c]
        who = k if half == 0 else nk
        cols = slice(c0, c0 + width)
        for i in range(2):
            row = pl.multiple_of(who * 512 + i * 256, 256)
            a = att[who, pl.ds(i * 256, 256)]
            for q in range(2):
                part[q, pl.ds(row, 256), pl.ds(c0, width)] = jnp.dot(
                    a[:, :128], OW[q, :, :, cols].reshape(128, width), preferred_element_type=F32
                ) + jnp.dot(
                    a[:, 128:], MO[q, :, :, cols].reshape(384, width), preferred_element_type=F32
                )

    for c, (_, _, width) in enumerate(CHUNKS):
        pair = (("o", c), ("m", c))
        for half in range(2):
            deps = [("image", 1)]
            deps += [("x", w, q, d) for w in pair for q in range(2) for d in (1, -1)]
            deps += [("terms", c, 0)] if half else []
            deps += [("terms", c - 1, 1)] if c else []
            takes = (x_last(pair[0]) + x_last(pair[1])) if half == 0 else []
            if c == 0 and half == 1:
                takes = [
                    (("att", i), lambda i=i: att.at[nk, pl.ds(i * IMAGE, IMAGE)]) for i in range(2)
                ]
            task(
                ("terms", c, half), takes=takes, deps=deps, prio=9, work=1.44 * width / 768,
                body=lambda c=c, half=half: output_terms(c, half),
            )

    half = BLOCK // 2

    def term(c, r, dz):
        row = pl.multiple_of((zn[dz % NZ] * 2 + rel_h[r]) * BLOCK, BLOCK)
        return part.at[rel_l[r], pl.ds(row, BLOCK), pl.ds(*CHUNKS[c][1:])]

    def reduction(c):
        kind, _, width = CHUNKS[c]
        zs, zr, ns, nr, ms, mr = chunk_refs[6 * c : 6 * c + 6]
        block, groups = BLOCK * width * 2, (1 if kind == "y" else 4)
        work = 0.05 + 0.12 * width / HALF
        ready = ("terms", c, 1)

        def along_z(g, r, d, dist):
            slot, landing = zs.at[g, 0 if d == 1 else 1, dist - 1], zr.at[g, 0 if d == 1 else 1, dist - 1]
            if dist == 4:
                slot, landing = slot.at[pl.ds(0, half)], landing.at[pl.ds(0, half)]
            before = zr.at[g, 0 if d == 1 else 1, min(dist, 3)]
            if dist == 3:
                before = before.at[pl.ds(0, half)]
            lo = 0 if d == 1 else half

            def body():
                blk = term(c, r, d * dist)
                if dist == 4:
                    slot[...] = blk[pl.ds(lo, half)].astype(BF16)
                elif dist == 3:
                    slot[pl.ds(half - lo, half)] = blk[pl.ds(half - lo, half)].astype(BF16)
                    slot[pl.ds(lo, half)] = (
                        blk[pl.ds(lo, half)] + before[...].astype(F32)
                    ).astype(BF16)
                else:
                    slot[...] = (blk[...] + before[...].astype(F32)).astype(BF16)

            from_y = ("y_end", c, (d * dist) % NZ) if kind == "y" else ready
            prio = 3 if kind == "y" else 8 - dist * 0.5 + (0 if r in (2, 3) else 0.3)
            task(
                ("c", c, r, d, dist), body=body, work=work, prio=prio + c * 0.01,
                takes=[] if dist == 4 else [(("c", c, r, d, dist + 1), lambda: before)],
                deps=[from_y] + ([] if dist == 4 else [("c", c, r, d, dist + 1)]),
                pushes=[
                    (("c", c, r, d, dist), ("z", d), block // 2 if dist == 4 else block,
                     lambda: (slot, landing, at_z(d)))
                ],
            )

        def z_end(g, r):
            def body():
                blk = term(c, r, 0)
                blk[...] = blk[...] + zr[g, 0, 0].astype(F32) + zr[g, 1, 0].astype(F32)
            task(
                ("z_end", c, r), body=body, work=work, prio=2,
                takes=[(("c", c, r, d, 1), lambda i=i: zr.at[g, i, 0]) for i, d in enumerate((1, -1))],
                deps=[("c", c, r, d, 1) for d in (1, -1)] + ([("y_end", c, 0)] if kind == "y" else []),
            )

        def along_y(g, dz, deps_out, deps_mid, deps_end, prios):
            tree = (c + dz) % 2
            far, near = ((flip_lh, "n"), (flip_l, "l")) if tree == 0 else ((flip_l, "l"), (flip_lh, "n"))
            direct, mid = (2, 1) if tree == 0 else (1, 2)

            def out_body():
                for j, r in enumerate((direct, 3)):
                    ns[g, j] = term(c, r, dz)[...].astype(BF16)

            def mid_body():
                ms[g] = (term(c, mid, dz)[...] + nr[g, 1].astype(F32)).astype(BF16)

            def end_body():
                blk = term(c, 0, dz)
                blk[...] = blk[...] + nr[g, 0].astype(F32) + mr[g].astype(F32)

            task(
                ("y_out", c, dz), body=out_body, deps=deps_out(direct), prio=prios[0],
                work=0.05 + 0.15 * width / HALF,
                pushes=[
                    (("n", c, dz, j), far[1], block, lambda j=j: (ns.at[g, j], nr.at[g, j], far[0]))
                    for j in (1, 0)
                ],
            )
            task(
                ("y_mid", c, dz), body=mid_body, work=work, prio=prios[1],
                takes=[(("n", c, dz, 1), lambda: nr.at[g, 1])],
                deps=[("y_out", c, dz)] + deps_mid(mid),
                pushes=[(("m", c, dz), near[1], block, lambda: (ms.at[g], mr.at[g], near[0]))],
            )
            task(
                ("y_end", c, dz), body=end_body, work=work, prio=prios[2],
                takes=[(("n", c, dz, 0), lambda: nr.at[g, 0]), (("m", c, dz), lambda: mr.at[g])],
                deps=[("y_mid", c, dz)] + deps_end,
            )

        if kind == "y":
            for dz in range(NZ):
                far = min(dz, NZ - dz)
                along_y(
                    dz, dz, lambda r: [ready], lambda r: [], [],
                    (20 - far, 4 - far * 0.1, 5 - far * 0.1),
                )
        for g in range(groups):
            for d in (1, -1):
                for dist in (4, 3, 2, 1):
                    along_z(g, g, d, dist)
            z_end(g, g)
        if kind == "z":
            along_y(
                0, 0, lambda r: [("z_end", c, r), ("z_end", c, 3)], lambda r: [("z_end", c, r)],
                [("z_end", c, 0)], (1, 1, 1),
            )

    for c in range(n):
        reduction(c)

    assert sorted(ORDER) == list(range(len(tasks)))
    for step in [tasks[i] for i in ORDER]:
        for key, ref in step.takes:
            take(key, ref())
        if step.body is not None:
            step.body()
        for key, _, _, refs in step.pushes:
            push(key, *refs())

    own = pl.ds(pl.multiple_of((z * 2 + yh) * BLOCK, BLOCK), BLOCK)
    g = out_bias[...].astype(F32)
    out[...] = part[yl, own] + jnp.concatenate([g[i : i + 1] for i in range(PIECE // 128)], axis=1)
    for copy in started:
        copy.wait_send()
    assert len(index) <= N_SEMS, len(index)


def per_device(
    tokens, ln_gain, qkv_weight, q_gain, k_gain, out_weight, mlp_in, mlp_bias, mlp_out, out_bias
):
    wq = jnp.transpose(qkv_weight, (1, 2, 3, 0))
    wm = jnp.transpose(mlp_in).reshape(2, UNITS, PIECE)
    mo = mlp_out.reshape(2, UNITS, PIECE)
    vm, hbm = pl.BlockSpec(memory_space=pltpu.VMEM), pl.BlockSpec(memory_space=pltpu.HBM)
    scratch = [
        pltpu.VMEM((BLOCK, PIECE), BF16),
        pltpu.VMEM((8, 128), F32),
        pltpu.VMEM((3, 8, 128), F32),
        pltpu.VMEM((2, 2, ROWS, HALF), BF16),
        pltpu.VMEM((2, 3, NX, 32, PIECE), BF16),
        pltpu.VMEM((2, NX, UNITS, PIECE), BF16),
        pltpu.VMEM((256, 128), BF16),
        pltpu.VMEM((NX, UNITS, 128), BF16),
        pltpu.VMEM((2, NX, 32, PIECE), BF16),
        pltpu.VMEM((2, NX, UNITS, PIECE), BF16),
        pltpu.VMEM((ROWS, 384), F32),
        pltpu.VMEM((ROWS, 384), F32),
        pltpu.VMEM((512, 384), F32),
        pltpu.VMEM((512, 384), F32),
        pltpu.VMEM((2, 512, 512), BF16),
        pltpu.VMEM((2, ROWS, PIECE), F32),
    ]
    for kind, _, width in CHUNKS:
        block = (BLOCK, width)
        groups, ys = (1, NZ) if kind == "y" else (4, 1)
        scratch += [pltpu.VMEM((groups, 2, 4, *block), BF16)] * 2
        scratch += [pltpu.VMEM((ys, 2, *block), BF16)] * 2
        scratch += [pltpu.VMEM((ys, *block), BF16)] * 2
    scratch += [
        pltpu.SemaphoreType.DMA((N_SEMS,)),
        pltpu.SemaphoreType.DMA((N_SEMS,)),
        pltpu.SemaphoreType.DMA((5,)),
    ]
    sums = pl.pallas_call(
        kernel,
        out_shape=jax.ShapeDtypeStruct((BLOCK, PIECE), F32),
        in_specs=[hbm, vm, hbm, hbm, vm, vm, hbm, vm, hbm, vm],
        out_specs=vm,
        scratch_shapes=scratch,
        compiler_params=pltpu.CompilerParams(
            collective_id=0, has_side_effects=True, vmem_limit_bytes=60 * 1024 * 1024
        ),
        name="layer",
    )(
        tokens, ln_gain.reshape(PIECE // 128, 128), wq, wm, q_gain.reshape(1, HD),
        k_gain.reshape(1, HD), out_weight, mlp_bias, mo,
        out_bias.reshape(PIECE // 128, 128),
    )
    return tokens.astype(F32) + sums


def solution(mesh):
    split = Mesh(
        mesh.devices.reshape(NX, 2, 2, NZ, 2), ("x", "yl", "k", "z", "yh")
    )
    token_axes, row, col = ("x", "z", "yh"), ("yl", "k"), ("z", "yh")
    placed = (
        P(token_axes, row),
        P(row),
        P(row, None, col, "x"),
        P(),
        P(),
        P(col, "x", row),
        P(row, token_axes),
        P(token_axes),
        P(token_axes, row),
        P(row),
    )
    return jax.shard_map(
        per_device, mesh=split, in_specs=placed, out_specs=P(token_axes, row), check_vma=False
    )
```

```python
import jax
import jax.numpy as jnp
from jax import lax
from jax.experimental import pallas as pl
from jax.experimental.pallas import tpu as pltpu
from jax.sharding import Mesh
from jax.sharding import PartitionSpec as P

D = 6144
HD = 128
IMAGE = 256
NX, NZ = 4, 8
BLOCK = 64
ROWS = 1024
PIECE = 1536
HALF = 768
UNITS = 96
EPS = 1e-06
MESH = pl.DeviceIdType.MESH
F32, BF16 = jnp.float32, jnp.bfloat16
NT = (((1,), (1,)), ((), ()))


CHUNKS = (("y", 0, 256), ("z", 256, 256), ("y", 512, 384), ("z", 896, 384), ("y", 1280, 256))
N_SEMS = 360
LAGS = ((2, (0, 1)),)
LINK_RATE, LATENCY, ISSUE = 44e3, 2.3, 0.03

ORDER = (
    0, 1, 69, 58, 2, 3, 57, 68, 4, 7, 46, 79, 44, 49, 48, 43, 35, 5, 10, 8, 47, 53, 54, 71, 72, 25, 13, 60, 61, 45,
    22, 6, 9, 16, 19, 11, 26, 42, 28, 36, 31, 14, 23, 34, 90, 101, 51, 50, 52, 59, 70, 17, 20, 27, 12, 41, 29, 32,
    37, 112, 24, 15, 40, 113, 21, 18, 38, 114, 39, 55, 56, 80, 81, 65, 64, 75, 76, 62, 63, 30, 33, 66, 67, 73, 74,
    78, 77, 91, 92, 115, 116, 117, 83, 82, 118, 119, 120, 87, 86, 121, 122, 123, 124, 84, 85, 89, 88, 125, 126,
    127, 128, 168, 199, 144, 147, 177, 190, 94, 93, 181, 195, 153, 172, 156, 135, 141, 150, 138, 186, 98, 95, 97,
    96, 169, 200, 99, 100, 102, 103, 145, 178, 148, 191, 196, 182, 173, 187, 157, 154, 129, 170, 201, 130, 179,
    192, 136, 151, 222, 216, 219, 139, 197, 183, 131, 188, 174, 132, 267, 271, 149, 104, 109, 108, 105, 213, 146,
    142, 225, 253, 249, 163, 262, 244, 159, 107, 106, 258, 240, 158, 202, 155, 110, 111, 152, 137, 193, 198, 184,
    189, 180, 175, 171, 220, 210, 272, 268, 250, 254, 164, 160, 133, 140, 259, 263, 134, 291, 217, 223, 297, 241,
    288, 245, 285, 294, 203, 194, 143, 185, 221, 235, 231, 176, 269, 273, 292, 226, 214, 300, 228, 282, 251, 255,
    289, 161, 218, 295, 211, 207, 264, 279, 224, 293, 298, 307, 303, 232, 236, 165, 260, 227, 286, 204, 270, 274,
    215, 252, 256, 290, 301, 296, 304, 242, 308, 246, 212, 233, 237, 229, 265, 261, 208, 283, 275, 257, 276, 280,
    299, 309, 166, 287, 305, 162, 302, 205, 247, 243, 230, 234, 238, 284, 209, 266, 277, 306, 310, 206, 167, 281,
    248, 239, 278, 311,
)


class Task:
    def __init__(self, name, takes=(), deps=(), work=0.02, body=None, pushes=(), prio=0.0):
        self.name, self.takes, self.deps, self.work = name, list(takes), list(deps), work
        self.body, self.pushes, self.prio = body, list(pushes), prio


def in_order(tasks):
    now, arrival, free, done, order, left = 0.0, {}, {}, set(), [], list(tasks)
    while left:
        best = None
        for task in left:
            if all(d in done for d in task.deps) and all(k in arrival for k, _ in task.takes):
                ready = max([now] + [arrival[k] for k, _ in task.takes])
                if best is None or (ready, task.prio) < best[:2]:
                    best = (ready, task.prio, task)
        now, _, task = best
        now += task.work
        for key, link, size, _ in task.pushes:
            now += ISSUE
            free[link] = max(now, free.get(link, 0.0)) + size / LINK_RATE
            arrival[key] = free[link] + LATENCY
        done.add(task.name)
        order.append(task)
        left.remove(task)
    return order


def kernel(
    tok_hbm, ln_gain, wq, wm, q_gain, k_gain, ow, bias_in, mo, out_bias,
    out,
    tok, stats, stats_in, xg, WQ, WM, BV, BI, OW, MO, hq, hm, hxq, hxm, att, part, *rest,
):
    chunk_refs, (send, recv, local) = rest[:-3], rest[-3:]
    x, yl, k = lax.axis_index("x"), lax.axis_index("yl"), lax.axis_index("k")
    z, yh = lax.axis_index("z"), lax.axis_index("yh")
    nl, nk, nh = 1 - yl, 1 - k, 1 - yh
    xs = [lax.rem(x + d, NX) for d in range(NX)]
    zn = [lax.rem(z + d, NZ) for d in range(NZ)]
    at_x = lambda d: {"x": xs[d % NX]}
    at_z = lambda d: {"z": zn[d % NZ]}
    flip_l, flip_lh = {"yl": nl}, {"yl": nl, "yh": nh}
    partner, flip_lk = {"k": nk}, {"yl": nl, "k": nk}
    rel_l, rel_h = (yl, nl, nl, yl), (yh, yh, nh, nh)

    index, started = {}, []

    def push(key, src, dst, peer):
        i = index.setdefault(key, len(index))
        copy = pltpu.make_async_remote_copy(
            src_ref=src, dst_ref=dst, send_sem=send.at[i], recv_sem=recv.at[i],
            device_id=peer, device_id_type=MESH,
        )
        copy.start()
        started.append(copy)

    def take(key, dst):
        i = index.setdefault(key, len(index))
        pltpu.make_async_remote_copy(
            src_ref=dst, dst_ref=dst, send_sem=send.at[i], recv_sem=recv.at[i],
            device_id=partner, device_id_type=MESH,
        ).wait_recv()

    tok_copy = pltpu.make_async_copy(tok_hbm, tok, local.at[4])
    tok_copy.start()
    barrier = pltpu.get_barrier_semaphore()
    peers = [at_x(1), at_x(-1), at_x(2), at_z(1), at_z(-1), flip_l, flip_lh, partner, flip_lk]
    for peer in peers:
        pl.semaphore_signal(barrier, inc=1, device_id=peer, device_id_type=MESH)

    tasks = []

    def task(*args, **kwargs):
        tasks.append(Task(*args, **kwargs))

    def cols_of(w):
        return pl.ds(*CHUNKS[w[1]][1:]) if isinstance(w, tuple) else pl.ds(0, PIECE)

    def stored(w, j, c=None):
        c = cols_of(w) if c is None else c
        if w == "q":
            return wq.at[:, j, :, c]
        return {"i": wm, "o": ow, "m": mo}[w[0]].at[j, :, c]

    def gathered(w, q, s, c=None):
        c = cols_of(w) if c is None else c
        if w == "q":
            return WQ.at[q, :, s, :, c]
        return {"i": WM, "o": OW, "m": MO}[w[0]].at[q, s, :, c]

    def part_of(w, q, s, d):
        lo = 0 if d == 1 else 1
        if w in ("q", "i"):
            return gathered(w, q, s, pl.ds(lo * HALF, HALF))
        rows = 16 if w[0] == "o" else 48
        ref = OW if w[0] == "o" else MO
        return ref.at[q, s, pl.ds(lo * rows, rows), cols_of(w)]

    def bytes_of(w):
        width = CHUNKS[w[1]][2] if isinstance(w, tuple) else PIECE
        return (32 if w[0] == "o" else UNITS) * width * 2

    quarter = (yl, nl)

    def x_push(w, q):
        def refs(d):
            dst = gathered(w, quarter[q], x)
            return (stored(w, yl) if q == 0 else dst), dst, at_x(d)
        return [(("x", w, q, d), ("x", d), bytes_of(w), lambda d=d: refs(d)) for d in (1, -1)]

    def w_push(w, h=None):
        c = None if h is None else pl.ds(h * HALF, HALF)
        size = bytes_of(w) if h is None else bytes_of(w) // 2
        return (("w", w, h), "l", size, lambda: (stored(w, nl, c), gathered(w, yl, x, c), flip_l))

    def w_take(w, h=None):
        c = None if h is None else pl.ds(h * HALF, HALF)
        return (("w", w, h), lambda: gathered(w, nl, x, c))

    def x_relay(w, q, deps):
        for d in (1, -1):
            def refs(d=d):
                ref = part_of(w, quarter[q], xs[-d % NX], d)
                return ref, ref, at_x(d)
            task(
                ("x", w, q, d), deps=deps, prio=-1,
                takes=[(("x", w, q, d), lambda d=d: gathered(w, quarter[q], xs[-d % NX]))],
                pushes=[(("x2", w, q, d), ("x", d), bytes_of(w) // 2, refs)],
            )

    def x_last(w):
        return [
            (("x2", w, q, d), lambda q=q, d=d: part_of(w, quarter[q], xs[2], d))
            for q in range(2) for d in (1, -1)
        ]

    def stats_push(i, peer, link):
        return (("stats", i), link, 8 * 128 * 4, lambda: (stats, stats_in.at[i], peer))

    local_copies = []

    def begin():
        pl.semaphore_wait(barrier, len(peers))
        for i, w in enumerate(("q", "i")):
            copy = pltpu.make_async_copy(stored(w, yl), gathered(w, yl, x), local.at[i])
            copy.start()
            local_copies.append(copy)
        for i, (src, dst) in enumerate(((ow, OW), (mo, MO))):
            copy = pltpu.make_async_copy(src.at[yl], dst.at[yl, x], local.at[2 + i])
            copy.start()
            local_copies.append(copy)

    def statistics():
        tok_copy.wait()
        t = tok[...].astype(F32)
        s1 = jnp.sum(t, 1, keepdims=True)
        s2 = jnp.sum(t * t, 1, keepdims=True)
        lane = lax.broadcasted_iota(jnp.int32, (BLOCK, 128), 1)
        both = jnp.where(lane < 64, s1, s2)
        turned = jnp.concatenate([both, both], axis=0).T
        row = lax.broadcasted_iota(jnp.int32, (8, 128), 0)
        stats[...] = jnp.where(row < 4, turned[0:1], turned[64:65])

    def bias_columns():
        for i, count in enumerate((128, 64)):
            b = bias_in[pl.ds(i * 128, count)].astype(F32).reshape(1, count)
            if count < 128:
                b = jnp.concatenate([b, b], axis=1)
            BV[pl.ds(i * 128, 128), :] = jnp.broadcast_to(b, (128, 128)).T.astype(BF16)
        mine = pl.ds(pl.multiple_of(yl * UNITS, 32), UNITS)
        BI[x] = BV[mine, :]

    def bias_refs(d):
        return BI.at[x], BI.at[x], at_x(d)

    def normalise():
        total = stats[...] + stats_in[0] + stats_in[1] + stats_in[2]
        mean = total[0:1] * (1.0 / D)
        var = total[4:5] * (1.0 / D) - mean * mean
        row = lax.broadcasted_iota(jnp.int32, (128, 128), 0)
        turned = jnp.where(row < 64, mean, lax.rsqrt(var + EPS)).T
        mean, scale = turned[:BLOCK, 0:1], turned[:BLOCK, 64:65]
        t = tok[...].astype(F32)
        g = ln_gain[...].astype(F32)
        g = jnp.concatenate([g[i : i + 1] for i in range(PIECE // 128)], axis=1)
        normed = ((t - mean) * scale * g).astype(BF16)
        own_row = pl.multiple_of((z * 2 + yh) * BLOCK, BLOCK)
        xg[0, yl, pl.ds(own_row, BLOCK)] = normed[:, :HALF]
        xg[1, yl, pl.ds(own_row, BLOCK)] = normed[:, HALF:]

    size = BLOCK * HALF * 2

    def tokens_at(h, r, dz):
        row = pl.multiple_of((zn[dz % NZ] * 2 + rel_h[r]) * BLOCK, BLOCK)
        return xg.at[h, rel_l[r], pl.ds(row, BLOCK)]

    def z_half(ref, d):
        return ref.at[pl.ds(0 if d == 1 else BLOCK // 2, BLOCK // 2)]

    def z_ref(h, r, d, dist, back):
        ref = tokens_at(h, r, -d * (dist - back))
        return z_half(ref, d) if dist == 4 else ref

    def z_push(h, r, d, dist):
        def refs():
            ref = z_ref(h, r, d, dist, 1)
            return ref, ref, at_z(d)
        return (("z", h, r, d, dist), ("z", d), size // 2 if dist == 4 else size, refs)

    def z_take(h, r, d, dist):
        return (("z", h, r, d, dist), lambda: z_ref(h, r, d, dist, 0))

    def y_copy(kind, h, r, dz, link, peer):
        def refs():
            ref = tokens_at(h, r, dz)
            return ref, ref, peer
        return ((kind, h, dz % NZ), link, size, refs)

    def y_push(h, dz):
        return [y_copy("yl", h, 0, dz, "l", flip_l), y_copy("yn", h, 0, dz, "n", flip_lh)]

    def y_take(kind, h, dz):
        r = {"yl": 1, "yn": 2, "yr": 3}[kind]
        return ((kind, h, dz % NZ), lambda: tokens_at(h, r, dz))

    def z_first(h, r):
        return [z_push(h, r, d, 1) for d in (1, -1)]

    task(("begin",), body=begin, pushes=x_push("q", 0), work=0.0, prio=-100)
    task(
        ("stats",), deps=[("begin",)], body=statistics, work=1.0, prio=-99,
        pushes=[stats_push(0, partner, "k"), stats_push(1, flip_l, "l"), stats_push(2, flip_lk, "l")]
        + [w_push("q", 0)] + x_push("i", 0),
    )
    task(
        ("bias",), deps=[("stats",)], body=bias_columns, work=0.3, prio=-98,
        pushes=[(("bias", d), "b", 0, lambda d=d: bias_refs(d)) for d in (1, -1, 2)],
    )
    task(
        ("norm",), deps=[("bias",)], body=normalise, work=0.8, prio=-97,
        takes=[(("stats", i), lambda i=i: stats_in.at[i]) for i in range(3)],
        pushes=z_first(0, 0) + z_first(1, 0) + y_push(1, 0) + y_push(0, 0)
        + [w_push("q", 1), w_push("i", 0)],
    )
    gather = []
    for h in range(2):
        for r in range(1 if h == 0 else 4):
            for d in (1, -1):
                for dist in (1, 2, 3):
                    task(
                        ("z", h, r, d, dist), deps=[("norm",)], prio=0 if h == 0 else 5,
                        takes=[z_take(h, r, d, dist)],
                        pushes=[z_push(h, r, d, dist + 1)] + (y_push(0, -d * dist) if h == 0 else []),
                    )
    task(("z4",), takes=[z_take(0, 0, 1, 4), z_take(0, 0, -1, 4)], pushes=y_push(0, 4))
    for dz in range(NZ):
        task(
            ("yl", 0, dz), deps=[("norm",)], prio=1, takes=[y_take("yl", 0, dz)],
            pushes=[y_copy("yr", 0, 1, dz, "n", flip_lh)],
        )
    task(
        ("yl", 1, 0), deps=[("norm",)], prio=1, takes=[y_take("yl", 1, 0)],
        pushes=[y_copy("yr", 1, 1, 0, "n", flip_lh)] + z_first(1, 1),
    )
    task(("yn", 1, 0), deps=[("norm",)], prio=2, takes=[y_take("yn", 1, 0)], pushes=z_first(1, 2))
    task(("yr", 1, 0), deps=[("norm",)], prio=2, takes=[y_take("yr", 1, 0)], pushes=z_first(1, 3))
    task(("w", "i", 1), deps=[("z", 0, 0, 1, 1)], prio=3, pushes=[w_push("i", 1)])
    for w in ("q", "i"):
        task(
            ("w", w), deps=[("norm",)] + ([("w", "i", 1)] if w == "i" else []), prio=2,
            takes=[w_take(w, 0), w_take(w, 1)], pushes=x_push(w, 1),
        )
        x_relay(w, 0, [("norm",)])
        x_relay(w, 1, [("w", w)])
    n = len(CHUNKS)
    for c in range(n):
        pair = (("o", c), ("m", c))
        if c == 0:
            after = [("z", 0, 0, 1, 3), ("z", 0, 0, -1, 3)]
        else:
            after = [("w2s", c - 1)] + ([("w2p", c - 2)] if c >= 2 else [])
        task(("w2s", c), deps=after, prio=6, pushes=[w_push(w) for w in pair])
        if c == 0:
            after = [("x", "i", 0, 1), ("x", "i", 0, -1), ("w", "i"), ("x", "q", 1, 1), ("x", "q", 1, -1)]
        else:
            after = [("w2q", c - 1)] + ([("x", "i", 1, 1), ("x", "i", 1, -1)] if c == 1 else [])
            for lag, qs in LAGS:
                if c >= lag:
                    after += [("x", (w, c - lag), q, d) for w in "om" for q in qs for d in (1, -1)]
        task(("w2p", c), deps=after, prio=7, pushes=x_push(pair[0], 0) + x_push(pair[1], 0))
        task(
            ("w2q", c), deps=[("w2s", c), ("w2p", c)], prio=7, takes=[w_take(w) for w in pair],
            pushes=x_push(pair[0], 1) + x_push(pair[1], 1),
        )
        for w in pair:
            x_relay(w, 0, [("w2p", c)])
            x_relay(w, 1, [("w2q", c)])
    first_relays = [t.name for t in tasks if t.name[0] in ("z", "z4", "yl", "yn", "yr", "w")]
    first_relays += [("x", w, q, d) for w in ("q", "i") for q in range(2) for d in (1, -1)]

    groups = ((0,), (1, -1), (2, -2), (3, -3), (4,))

    def rows_of(dzs):
        return [pl.ds(pl.multiple_of(zn[dz % NZ] * 128, 128), 128) for dz in dzs]

    def product(lhs, weights, h):
        cols = pl.ds(h * HALF, HALF)
        rhs = weights[..., cols].reshape(384, HALF)
        return lax.dot_general(lhs, rhs, NT, preferred_element_type=F32)

    def project(dzs):
        if dzs == (0,):
            for copy in local_copies[:2]:
                copy.wait()
        rows = rows_of(dzs)
        acc_q = jnp.zeros((128 * len(dzs), 384), F32)
        acc_m = jnp.zeros((128 * len(dzs), 384), F32)
        for h in range(2):
            for q in (yl, nl):
                lhs = jnp.concatenate([xg[h, q, r] for r in rows], axis=0)
                acc_q += product(lhs, WQ.at[q], h)
                if q is yl:
                    acc_m += product(lhs, WM.at[q], h)
        for i, r in enumerate(rows):
            hq[r] = acc_q[i * 128 : (i + 1) * 128]
            hm[r] = acc_m[i * 128 : (i + 1) * 128]

    def project_last(i):
        row = pl.ds(pl.multiple_of(lax.rem(i * 256 + nk * 512, ROWS), 256), 256)
        acc = hm[row]
        for h in range(2):
            acc += product(xg[h, nl, row], WM.at[nl], h)
        hm[row] = acc

    def hq_refs():
        return hq.at[pl.ds(pl.multiple_of(nk * 512, 512), 512)], hxq, partner

    def hm_refs(i):
        theirs = hm.at[pl.ds(pl.multiple_of(nk * 512 + i * 256, 256), 256)]
        return theirs, hxm.at[pl.ds(i * 256, 256)], partner

    k_scale = LINK_RATE / 600e3
    early = x_last("q") + [t for t in x_last("i") if t[0][2] == 0]
    late = [t for t in x_last("i") if t[0][2] == 1]
    early_relays = [("x", w, q, d) for w, q in (("q", 0), ("q", 1), ("i", 0)) for d in (1, -1)]
    late_relays = first_relays
    for g, dzs in enumerate(groups):
        takes, deps = (list(early), list(early_relays)) if g == 0 else ([], [("p", g - 1)])
        for dz in dzs:
            takes += [y_take(kind, 0, dz) for kind in ("yn", "yr")]
            deps += [("yl", 0, dz % NZ)]
            if dz == 0:
                deps += [("norm",), ("yl", 1, 0), ("yn", 1, 0), ("yr", 1, 0)]
            elif dz == 4:
                deps += [("z4",)]
                takes += [z_take(1, r, d, 4) for r in range(4) for d in (1, -1)]
            else:
                d = -1 if dz > 0 else 1
                deps += [("z", 0, 0, d, abs(dz))] + [("z", 1, r, d, abs(dz)) for r in range(4)]
        task(
            ("p", g), takes=takes, deps=deps, body=lambda dzs=dzs: project(dzs), prio=30,
            work=0.9 if len(dzs) == 1 else 1.4,
            pushes=[(("hq",), "k", 512 * 384 * 4 * k_scale, hq_refs)] if g == 4 else [],
        )
    for i in range(4):
        task(
            ("pl", i), takes=late if i == 0 else [],
            deps=late_relays + [("p", 4)] if i == 0 else [("pl", i - 1)],
            body=lambda i=i: project_last(i), work=0.5, prio=10,
            pushes=[(("hm", i), "k", 256 * 384 * 4 * k_scale, lambda i=i: hm_refs(i))] if i < 2 else [],
        )

    def head_norm(values, gain):
        centred = values - jnp.mean(values, -1, keepdims=True)
        spread = jnp.mean(centred * centred, -1, keepdims=True)
        return (centred * lax.rsqrt(spread + EPS) * gain[...].astype(F32)).astype(BF16)

    def own_rows(i):
        return pl.ds(pl.multiple_of(k * 512 + i * IMAGE, IMAGE), IMAGE)

    def attend(i):
        mine = pl.ds(i * IMAGE, IMAGE)
        joined = hq[own_rows(i)] + hxq[mine]
        q = head_norm(joined[:, 0:128], q_gain)
        kk = head_norm(joined[:, 128:256], k_gain)
        v = joined[:, 256:384].astype(BF16)
        scores = lax.dot_general(q, kk, NT, preferred_element_type=F32) * HD ** (-0.5)
        e = jnp.exp(scores - jnp.max(scores, -1, keepdims=True))
        probs = (e / jnp.sum(e, -1, keepdims=True)).astype(BF16)
        attended = jnp.dot(probs, v, preferred_element_type=F32)
        att[k, mine, pl.ds(0, 128)] = attended.astype(BF16)

    def activate(i):
        mine = pl.ds(i * IMAGE, IMAGE)
        unit = (lax.broadcasted_iota(jnp.int32, (IMAGE, 128), 1) == 0).astype(F32).astype(BF16)
        pre = hm[own_rows(i)] + hxm[mine] + lax.dot_general(
            unit, BI[...].reshape(384, 128), NT, preferred_element_type=F32
        )
        hidden = 0.5 * pre * (1.0 + lax.erf(pre * (0.5 ** 0.5)))
        att[k, mine, pl.ds(128, 384)] = hidden.astype(BF16)

    def att_refs(i):
        ref = att.at[k, pl.ds(i * IMAGE, IMAGE)]
        return ref, ref, partner

    for i in range(2):
        task(
            ("attend", i), deps=[("pl", 3)] + [("attend", 0)] * i, prio=10, work=0.45,
            takes=[(("hq",), lambda: hxq)] if i == 0 else [], body=lambda i=i: attend(i),
        )
    for i in range(2):
        takes = [(("hm", i), lambda i=i: hxm.at[pl.ds(i * 256, 256)])]
        if i == 0:
            takes += [(("bias", d), lambda d=d: BI.at[xs[-d % NX]]) for d in (1, -1, 2)]
        task(
            ("image", i), takes=takes, deps=[("attend", 1)] + [("image", 0)] * i, prio=10, work=0.45,
            body=lambda i=i: activate(i),
            pushes=[(("att", i), "k", 256 * 512 * 2 * k_scale, lambda i=i: att_refs(i))],
        )

    def output_terms(c, half):
        if c == 0 and half == 0:
            for copy in local_copies[2:]:
                copy.wait()
        _, c0, width = CHUNKS[c]
        who = k if half == 0 else nk
        cols = slice(c0, c0 + width)
        for i in range(2):
            row = pl.multiple_of(who * 512 + i * 256, 256)
            a = att[who, pl.ds(i * 256, 256)]
            for q in range(2):
                part[q, pl.ds(row, 256), pl.ds(c0, width)] = jnp.dot(
                    a[:, :128], OW[q, :, :, cols].reshape(128, width), preferred_element_type=F32
                ) + jnp.dot(
                    a[:, 128:], MO[q, :, :, cols].reshape(384, width), preferred_element_type=F32
                )

    for c, (_, _, width) in enumerate(CHUNKS):
        pair = (("o", c), ("m", c))
        for half in range(2):
            deps = [("image", 1)]
            deps += [("x", w, q, d) for w in pair for q in range(2) for d in (1, -1)]
            deps += [("terms", c, 0)] if half else []
            deps += [("terms", c - 1, 1)] if c else []
            takes = (x_last(pair[0]) + x_last(pair[1])) if half == 0 else []
            if c == 0 and half == 1:
                takes = [
                    (("att", i), lambda i=i: att.at[nk, pl.ds(i * IMAGE, IMAGE)]) for i in range(2)
                ]
            task(
                ("terms", c, half), takes=takes, deps=deps, prio=9, work=1.44 * width / 768,
                body=lambda c=c, half=half: output_terms(c, half),
            )

    half = BLOCK // 2

    def term(c, r, dz):
        row = pl.multiple_of((zn[dz % NZ] * 2 + rel_h[r]) * BLOCK, BLOCK)
        return part.at[rel_l[r], pl.ds(row, BLOCK), pl.ds(*CHUNKS[c][1:])]

    def reduction(c):
        kind, _, width = CHUNKS[c]
        zs, zr, ns, nr, ms, mr = chunk_refs[6 * c : 6 * c + 6]
        block, groups = BLOCK * width * 2, (1 if kind == "y" else 4)
        work = 0.05 + 0.12 * width / HALF
        ready = ("terms", c, 1)

        def along_z(g, r, d, dist):
            slot, landing = zs.at[g, 0 if d == 1 else 1, dist - 1], zr.at[g, 0 if d == 1 else 1, dist - 1]
            if dist == 4:
                slot, landing = slot.at[pl.ds(0, half)], landing.at[pl.ds(0, half)]
            before = zr.at[g, 0 if d == 1 else 1, min(dist, 3)]
            if dist == 3:
                before = before.at[pl.ds(0, half)]
            lo = 0 if d == 1 else half

            def body():
                blk = term(c, r, d * dist)
                if dist == 4:
                    slot[...] = blk[pl.ds(lo, half)].astype(BF16)
                elif dist == 3:
                    slot[pl.ds(half - lo, half)] = blk[pl.ds(half - lo, half)].astype(BF16)
                    slot[pl.ds(lo, half)] = (
                        blk[pl.ds(lo, half)] + before[...].astype(F32)
                    ).astype(BF16)
                else:
                    slot[...] = (blk[...] + before[...].astype(F32)).astype(BF16)

            from_y = ("y_end", c, (d * dist) % NZ) if kind == "y" else ready
            prio = 3 if kind == "y" else 8 - dist * 0.5 + (0 if r in (2, 3) else 0.3)
            task(
                ("c", c, r, d, dist), body=body, work=work, prio=prio + c * 0.01,
                takes=[] if dist == 4 else [(("c", c, r, d, dist + 1), lambda: before)],
                deps=[from_y] + ([] if dist == 4 else [("c", c, r, d, dist + 1)]),
                pushes=[
                    (("c", c, r, d, dist), ("z", d), block // 2 if dist == 4 else block,
                     lambda: (slot, landing, at_z(d)))
                ],
            )

        def z_end(g, r):
            def body():
                blk = term(c, r, 0)
                blk[...] = blk[...] + zr[g, 0, 0].astype(F32) + zr[g, 1, 0].astype(F32)
            task(
                ("z_end", c, r), body=body, work=work, prio=2,
                takes=[(("c", c, r, d, 1), lambda i=i: zr.at[g, i, 0]) for i, d in enumerate((1, -1))],
                deps=[("c", c, r, d, 1) for d in (1, -1)] + ([("y_end", c, 0)] if kind == "y" else []),
            )

        def along_y(g, dz, deps_out, deps_mid, deps_end, prios):
            tree = (c + dz) % 2
            far, near = ((flip_lh, "n"), (flip_l, "l")) if tree == 0 else ((flip_l, "l"), (flip_lh, "n"))
            direct, mid = (2, 1) if tree == 0 else (1, 2)

            def out_body():
                for j, r in enumerate((direct, 3)):
                    ns[g, j] = term(c, r, dz)[...].astype(BF16)

            def mid_body():
                ms[g] = (term(c, mid, dz)[...] + nr[g, 1].astype(F32)).astype(BF16)

            def end_body():
                blk = term(c, 0, dz)
                blk[...] = blk[...] + nr[g, 0].astype(F32) + mr[g].astype(F32)

            task(
                ("y_out", c, dz), body=out_body, deps=deps_out(direct), prio=prios[0],
                work=0.05 + 0.15 * width / HALF,
                pushes=[
                    (("n", c, dz, j), far[1], block, lambda j=j: (ns.at[g, j], nr.at[g, j], far[0]))
                    for j in (1, 0)
                ],
            )
            task(
                ("y_mid", c, dz), body=mid_body, work=work, prio=prios[1],
                takes=[(("n", c, dz, 1), lambda: nr.at[g, 1])],
                deps=[("y_out", c, dz)] + deps_mid(mid),
                pushes=[(("m", c, dz), near[1], block, lambda: (ms.at[g], mr.at[g], near[0]))],
            )
            task(
                ("y_end", c, dz), body=end_body, work=work, prio=prios[2],
                takes=[(("n", c, dz, 0), lambda: nr.at[g, 0]), (("m", c, dz), lambda: mr.at[g])],
                deps=[("y_mid", c, dz)] + deps_end,
            )

        if kind == "y":
            for dz in range(NZ):
                far = min(dz, NZ - dz)
                along_y(
                    dz, dz, lambda r: [ready], lambda r: [], [],
                    (20 - far, 4 - far * 0.1, 5 - far * 0.1),
                )
        for g in range(groups):
            for d in (1, -1):
                for dist in (4, 3, 2, 1):
                    along_z(g, g, d, dist)
            z_end(g, g)
        if kind == "z":
            along_y(
                0, 0, lambda r: [("z_end", c, r), ("z_end", c, 3)], lambda r: [("z_end", c, r)],
                [("z_end", c, 0)], (1, 1, 1),
            )

    for c in range(n):
        reduction(c)

    assert sorted(ORDER) == list(range(len(tasks)))
    for step in [tasks[i] for i in ORDER]:
        for key, ref in step.takes:
            take(key, ref())
        if step.body is not None:
            step.body()
        for key, _, _, refs in step.pushes:
            push(key, *refs())

    own = pl.ds(pl.multiple_of((z * 2 + yh) * BLOCK, BLOCK), BLOCK)
    g = out_bias[...].astype(F32)
    out[...] = part[yl, own] + jnp.concatenate([g[i : i + 1] for i in range(PIECE // 128)], axis=1)
    for copy in started:
        copy.wait_send()
    assert len(index) <= N_SEMS, len(index)


def per_device(
    tokens, ln_gain, qkv_weight, q_gain, k_gain, out_weight, mlp_in, mlp_bias, mlp_out, out_bias
):
    wq = jnp.transpose(qkv_weight, (1, 2, 3, 0))
    wm = jnp.transpose(mlp_in).reshape(2, UNITS, PIECE)
    mo = mlp_out.reshape(2, UNITS, PIECE)
    vm, hbm = pl.BlockSpec(memory_space=pltpu.VMEM), pl.BlockSpec(memory_space=pltpu.HBM)
    scratch = [
        pltpu.VMEM((BLOCK, PIECE), BF16),
        pltpu.VMEM((8, 128), F32),
        pltpu.VMEM((3, 8, 128), F32),
        pltpu.VMEM((2, 2, ROWS, HALF), BF16),
        pltpu.VMEM((2, 3, NX, 32, PIECE), BF16),
        pltpu.VMEM((2, NX, UNITS, PIECE), BF16),
        pltpu.VMEM((256, 128), BF16),
        pltpu.VMEM((NX, UNITS, 128), BF16),
        pltpu.VMEM((2, NX, 32, PIECE), BF16),
        pltpu.VMEM((2, NX, UNITS, PIECE), BF16),
        pltpu.VMEM((ROWS, 384), F32),
        pltpu.VMEM((ROWS, 384), F32),
        pltpu.VMEM((512, 384), F32),
        pltpu.VMEM((512, 384), F32),
        pltpu.VMEM((2, 512, 512), BF16),
        pltpu.VMEM((2, ROWS, PIECE), F32),
    ]
    for kind, _, width in CHUNKS:
        block = (BLOCK, width)
        groups, ys = (1, NZ) if kind == "y" else (4, 1)
        scratch += [pltpu.VMEM((groups, 2, 4, *block), BF16)] * 2
        scratch += [pltpu.VMEM((ys, 2, *block), BF16)] * 2
        scratch += [pltpu.VMEM((ys, *block), BF16)] * 2
    scratch += [
        pltpu.SemaphoreType.DMA((N_SEMS,)),
        pltpu.SemaphoreType.DMA((N_SEMS,)),
        pltpu.SemaphoreType.DMA((5,)),
    ]
    sums = pl.pallas_call(
        kernel,
        out_shape=jax.ShapeDtypeStruct((BLOCK, PIECE), F32),
        in_specs=[hbm, vm, hbm, hbm, vm, vm, hbm, vm, hbm, vm],
        out_specs=vm,
        scratch_shapes=scratch,
        compiler_params=pltpu.CompilerParams(
            collective_id=0, has_side_effects=True, vmem_limit_bytes=60 * 1024 * 1024
        ),
        name="layer",
    )(
        tokens, ln_gain.reshape(PIECE // 128, 128), wq, wm, q_gain.reshape(1, HD),
        k_gain.reshape(1, HD), out_weight, mlp_bias, mo,
        out_bias.reshape(PIECE // 128, 128),
    )
    return tokens.astype(F32) + sums


def solution(mesh):
    split = Mesh(
        mesh.devices.reshape(NX, 2, 2, NZ, 2), ("x", "yl", "k", "z", "yh")
    )
    token_axes, row, col = ("x", "z", "yh"), ("yl", "k"), ("z", "yh")
    placed = (
        P(token_axes, row),
        P(row),
        P(row, None, col, "x"),
        P(),
        P(),
        P(col, "x", row),
        P(row, token_axes),
        P(token_axes),
        P(token_axes, row),
        P(row),
    )
    return jax.shard_map(
        per_device, mesh=split, in_specs=placed, out_specs=P(token_axes, row), check_vma=False
    )
```

```python
import jax
import jax.numpy as jnp
from jax import lax
from jax.experimental import pallas as pl
from jax.experimental.pallas import tpu as pltpu
from jax.sharding import Mesh
from jax.sharding import PartitionSpec as P

D = 6144
HD = 128
IMAGE = 256
NX, NZ = 4, 8
BLOCK = 64
ROWS = 1024
PIECE = 1536
HALF = 768
UNITS = 96
EPS = 1e-06
MESH = pl.DeviceIdType.MESH
F32, BF16 = jnp.float32, jnp.bfloat16
NT = (((1,), (1,)), ((), ()))


CHUNKS = (("y", 0, 256), ("z", 256, 256), ("y", 512, 384), ("z", 896, 384), ("y", 1280, 256))
N_SEMS = 400
LAGS = ((2, (0, 1)),)
LINK_RATE, LATENCY, ISSUE = 44e3, 2.3, 0.03

ORDER = (
    0, 1, 4, 5, 2, 3, 7, 8, 13, 6, 55, 14, 110, 53, 56, 57, 58, 52, 15, 16, 9, 19, 10, 22, 44, 63, 62, 31, 34, 51,
    54, 28, 25, 17, 11, 12, 18, 66, 77, 59, 60, 23, 20, 61, 78, 67, 32, 45, 37, 40, 35, 29, 26, 46, 50, 21, 24,
    121, 49, 123, 41, 47, 43, 88, 99, 38, 33, 36, 65, 64, 68, 79, 89, 80, 81, 30, 27, 125, 84, 85, 70, 69, 48, 74,
    73, 39, 42, 127, 122, 71, 72, 124, 126, 75, 76, 90, 128, 82, 83, 129, 86, 87, 100, 101, 92, 91, 130, 96, 95,
    131, 132, 133, 134, 93, 94, 135, 97, 98, 136, 137, 138, 209, 196, 157, 160, 187, 200, 102, 191, 103, 151, 145,
    178, 163, 154, 205, 182, 148, 107, 106, 104, 105, 210, 197, 188, 158, 166, 161, 201, 109, 108, 192, 111, 112,
    179, 183, 206, 152, 155, 139, 211, 198, 140, 202, 189, 146, 149, 229, 164, 232, 159, 226, 169, 193, 173, 180,
    141, 184, 167, 114, 113, 235, 207, 223, 142, 281, 277, 263, 118, 117, 259, 268, 272, 254, 162, 250, 156, 153,
    115, 116, 199, 119, 120, 150, 190, 203, 147, 194, 165, 181, 230, 238, 185, 208, 212, 278, 282, 170, 264, 174,
    260, 168, 143, 269, 273, 144, 255, 251, 304, 301, 227, 233, 307, 295, 289, 298, 204, 195, 186, 231, 245, 241,
    213, 283, 279, 302, 224, 236, 310, 220, 292, 265, 305, 261, 228, 299, 239, 217, 270, 274, 234, 308, 303, 317,
    313, 242, 246, 296, 225, 214, 284, 280, 237, 266, 290, 175, 262, 252, 311, 306, 318, 256, 221, 300, 314, 171,
    247, 275, 243, 271, 240, 285, 293, 267, 286, 218, 309, 319, 312, 176, 297, 315, 253, 215, 257, 222, 172, 294,
    244, 291, 248, 276, 287, 320, 316, 216, 219, 258, 177, 288, 249, 321,
)


class Task:
    def __init__(self, name, takes=(), deps=(), work=0.02, body=None, pushes=(), prio=0.0):
        self.name, self.takes, self.deps, self.work = name, list(takes), list(deps), work
        self.body, self.pushes, self.prio = body, list(pushes), prio


def in_order(tasks):
    now, arrival, free, done, order, left = 0.0, {}, {}, set(), [], list(tasks)
    while left:
        best = None
        for task in left:
            if all(d in done for d in task.deps) and all(k in arrival for k, _ in task.takes):
                ready = max([now] + [arrival[k] for k, _ in task.takes])
                if best is None or (ready, task.prio) < best[:2]:
                    best = (ready, task.prio, task)
        now, _, task = best
        now += task.work
        for key, link, size, _ in task.pushes:
            now += ISSUE
            free[link] = max(now, free.get(link, 0.0)) + size / LINK_RATE
            arrival[key] = free[link] + LATENCY
        done.add(task.name)
        order.append(task)
        left.remove(task)
    return order


def kernel(
    tok_hbm, ln_gain, wq, wm, q_gain, k_gain, ow, bias_in, mo, out_bias,
    out,
    tok, stats, stats_in, xg, WQ, WM, BV, BI, OW, MO, hq, hm, hxq, hxm, att, part, *rest,
):
    chunk_refs, (send, recv, local) = rest[:-3], rest[-3:]
    x, yl, k = lax.axis_index("x"), lax.axis_index("yl"), lax.axis_index("k")
    z, yh = lax.axis_index("z"), lax.axis_index("yh")
    nl, nk, nh = 1 - yl, 1 - k, 1 - yh
    xs = [lax.rem(x + d, NX) for d in range(NX)]
    zn = [lax.rem(z + d, NZ) for d in range(NZ)]
    at_x = lambda d: {"x": xs[d % NX]}
    at_z = lambda d: {"z": zn[d % NZ]}
    flip_l, flip_lh = {"yl": nl}, {"yl": nl, "yh": nh}
    partner, flip_lk = {"k": nk}, {"yl": nl, "k": nk}
    rel_l, rel_h = (yl, nl, nl, yl), (yh, yh, nh, nh)

    index, started = {}, []

    def push(key, src, dst, peer):
        i = index.setdefault(key, len(index))
        copy = pltpu.make_async_remote_copy(
            src_ref=src, dst_ref=dst, send_sem=send.at[i], recv_sem=recv.at[i],
            device_id=peer, device_id_type=MESH,
        )
        copy.start()
        started.append(copy)

    def take(key, dst):
        i = index.setdefault(key, len(index))
        pltpu.make_async_remote_copy(
            src_ref=dst, dst_ref=dst, send_sem=send.at[i], recv_sem=recv.at[i],
            device_id=partner, device_id_type=MESH,
        ).wait_recv()

    tok_copy = pltpu.make_async_copy(tok_hbm, tok, local.at[4])
    tok_copy.start()
    barrier = pltpu.get_barrier_semaphore()
    peers = [at_x(1), at_x(-1), at_x(2), at_z(1), at_z(-1), flip_l, flip_lh, partner, flip_lk]
    for peer in peers:
        pl.semaphore_signal(barrier, inc=1, device_id=peer, device_id_type=MESH)

    tasks = []

    def task(*args, **kwargs):
        tasks.append(Task(*args, **kwargs))

    def cols_of(w):
        return pl.ds(*CHUNKS[w[1]][1:]) if isinstance(w, tuple) else pl.ds(0, PIECE)

    def stored(w, j, c=None):
        c = cols_of(w) if c is None else c
        if w == "q":
            return wq.at[:, j, :, c]
        return {"i": wm, "o": ow, "m": mo}[w[0]].at[j, :, c]

    def gathered(w, q, s, c=None):
        c = cols_of(w) if c is None else c
        if w == "q":
            return WQ.at[q, :, s, :, c]
        return {"i": WM, "o": OW, "m": MO}[w[0]].at[q, s, :, c]

    def part_of(w, q, s, d):
        lo = 0 if d == 1 else 1
        if w in ("q", "i"):
            return gathered(w, q, s, pl.ds(lo * HALF, HALF))
        rows = 16 if w[0] == "o" else 48
        ref = OW if w[0] == "o" else MO
        return ref.at[q, s, pl.ds(lo * rows, rows), cols_of(w)]

    def bytes_of(w):
        width = CHUNKS[w[1]][2] if isinstance(w, tuple) else PIECE
        return (32 if w[0] == "o" else UNITS) * width * 2

    quarter = (yl, nl)

    def x_push(w, q):
        def refs(d):
            dst = gathered(w, quarter[q], x)
            return (stored(w, yl) if q == 0 else dst), dst, at_x(d)
        return [(("x", w, q, d), ("x", d), bytes_of(w), lambda d=d: refs(d)) for d in (1, -1)]

    def w_push(w, h=None):
        c = None if h is None else pl.ds(h * HALF, HALF)
        size = bytes_of(w) if h is None else bytes_of(w) // 2
        return (("w", w, h), "l", size, lambda: (stored(w, nl, c), gathered(w, yl, x, c), flip_l))

    def w_take(w, h=None):
        c = None if h is None else pl.ds(h * HALF, HALF)
        return (("w", w, h), lambda: gathered(w, nl, x, c))

    def x_relay(w, q, deps):
        for d in (1, -1):
            def refs(d=d):
                ref = part_of(w, quarter[q], xs[-d % NX], d)
                return ref, ref, at_x(d)
            task(
                ("x", w, q, d), deps=deps, prio=-1,
                takes=[(("x", w, q, d), lambda d=d: gathered(w, quarter[q], xs[-d % NX]))],
                pushes=[(("x2", w, q, d), ("x", d), bytes_of(w) // 2, refs)],
            )

    def x_last(w):
        return [
            (("x2", w, q, d), lambda q=q, d=d: part_of(w, quarter[q], xs[2], d))
            for q in range(2) for d in (1, -1)
        ]

    def stats_push(i, peer, link):
        return (("stats", i), link, 8 * 128 * 4, lambda: (stats, stats_in.at[i], peer))

    local_copies = []

    def begin():
        pl.semaphore_wait(barrier, len(peers))
        for i, w in enumerate(("q", "i")):
            copy = pltpu.make_async_copy(stored(w, yl), gathered(w, yl, x), local.at[i])
            copy.start()
            local_copies.append(copy)
        for i, (src, dst) in enumerate(((ow, OW), (mo, MO))):
            copy = pltpu.make_async_copy(src.at[yl], dst.at[yl, x], local.at[2 + i])
            copy.start()
            local_copies.append(copy)

    def statistics():
        tok_copy.wait()
        t = tok[...].astype(F32)
        s1 = jnp.sum(t, 1, keepdims=True)
        s2 = jnp.sum(t * t, 1, keepdims=True)
        lane = lax.broadcasted_iota(jnp.int32, (BLOCK, 128), 1)
        both = jnp.where(lane < 64, s1, s2)
        turned = jnp.concatenate([both, both], axis=0).T
        row = lax.broadcasted_iota(jnp.int32, (8, 128), 0)
        stats[...] = jnp.where(row < 4, turned[0:1], turned[64:65])

    def bias_columns():
        for i, count in enumerate((128, 64)):
            b = bias_in[pl.ds(i * 128, count)].astype(F32).reshape(1, count)
            if count < 128:
                b = jnp.concatenate([b, b], axis=1)
            BV[pl.ds(i * 128, 128), :] = jnp.broadcast_to(b, (128, 128)).T.astype(BF16)
        mine = pl.ds(pl.multiple_of(yl * UNITS, 32), UNITS)
        BI[x] = BV[mine, :]

    def bias_refs(d):
        return BI.at[x], BI.at[x], at_x(d)

    def normalise():
        total = stats[...] + stats_in[0] + stats_in[1] + stats_in[2]
        mean = total[0:1] * (1.0 / D)
        var = total[4:5] * (1.0 / D) - mean * mean
        row = lax.broadcasted_iota(jnp.int32, (128, 128), 0)
        turned = jnp.where(row < 64, mean, lax.rsqrt(var + EPS)).T
        mean, scale = turned[:BLOCK, 0:1], turned[:BLOCK, 64:65]
        t = tok[...].astype(F32)
        g = ln_gain[...].astype(F32)
        g = jnp.concatenate([g[i : i + 1] for i in range(PIECE // 128)], axis=1)
        normed = ((t - mean) * scale * g).astype(BF16)
        own_row = pl.multiple_of((z * 2 + yh) * BLOCK, BLOCK)
        xg[0, yl, pl.ds(own_row, BLOCK)] = normed[:, :HALF]
        xg[1, yl, pl.ds(own_row, BLOCK)] = normed[:, HALF:]

    size = BLOCK * HALF * 2

    def tokens_at(h, r, dz):
        row = pl.multiple_of((zn[dz % NZ] * 2 + rel_h[r]) * BLOCK, BLOCK)
        return xg.at[h, rel_l[r], pl.ds(row, BLOCK)]

    def z_half(ref, d):
        return ref.at[pl.ds(0 if d == 1 else BLOCK // 2, BLOCK // 2)]

    def z_ref(h, r, d, dist, back):
        ref = tokens_at(h, r, -d * (dist - back))
        return z_half(ref, d) if dist == 4 else ref

    def z_push(h, r, d, dist):
        def refs():
            ref = z_ref(h, r, d, dist, 1)
            return ref, ref, at_z(d)
        return (("z", h, r, d, dist), ("z", d), size // 2 if dist == 4 else size, refs)

    def z_take(h, r, d, dist):
        return (("z", h, r, d, dist), lambda: z_ref(h, r, d, dist, 0))

    def y_copy(kind, h, r, dz, link, peer):
        def refs():
            ref = tokens_at(h, r, dz)
            return ref, ref, peer
        return ((kind, h, dz % NZ), link, size, refs)

    def y_push(h, dz):
        return [y_copy("yl", h, 0, dz, "l", flip_l), y_copy("yn", h, 0, dz, "n", flip_lh)]

    def y_take(kind, h, dz):
        r = {"yl": 1, "yn": 2, "yr": 3}[kind]
        return ((kind, h, dz % NZ), lambda: tokens_at(h, r, dz))

    def z_first(h, r):
        return [z_push(h, r, d, 1) for d in (1, -1)]

    task(("begin",), body=begin, pushes=x_push("q", 0), work=0.0, prio=-100)
    task(
        ("stats",), deps=[("begin",)], body=statistics, work=1.0, prio=-99,
        pushes=[stats_push(0, partner, "k"), stats_push(1, flip_l, "l"), stats_push(2, flip_lk, "l")]
        + [w_push("q", 0)],
    )
    task(
        ("bias",), deps=[("stats",)], body=bias_columns, work=0.3, prio=-98,
        pushes=[(("bias", d), "b", 0, lambda d=d: bias_refs(d)) for d in (1, -1, 2)],
    )
    task(
        ("norm",), deps=[("bias",)], body=normalise, work=0.8, prio=-97,
        takes=[(("stats", i), lambda i=i: stats_in.at[i]) for i in range(3)],
        pushes=z_first(0, 0) + z_first(1, 0) + y_push(1, 0) + y_push(0, 0),
    )
    task(("xp", "i"), deps=[("stats",)], prio=-98.5, pushes=x_push("i", 0))
    task(("w", "q", 1), deps=[("norm",)], prio=-90, pushes=[w_push("q", 1)])
    task(("w", "i", 0), deps=[("w", "q", 1)], prio=-89, pushes=[w_push("i", 0)])
    for h in range(2):
        for r in range(1 if h == 0 else 4):
            for d in (1, -1):
                for dist in (1, 2, 3):
                    task(
                        ("z", h, r, d, dist), deps=[("norm",)], prio=0 if h == 0 else 5,
                        takes=[z_take(h, r, d, dist)],
                        pushes=[z_push(h, r, d, dist + 1)],
                    )
                    if h == 0:
                        task(
                            ("yp", (-d * dist) % NZ), deps=[("z", h, r, d, dist)], prio=0,
                            pushes=y_push(0, -d * dist),
                        )
    task(("z4",), takes=[z_take(0, 0, 1, 4), z_take(0, 0, -1, 4)], pushes=y_push(0, 4))
    for dz in range(NZ):
        task(
            ("yl", 0, dz), deps=[("norm",)], prio=1, takes=[y_take("yl", 0, dz)],
            pushes=[y_copy("yr", 0, 1, dz, "n", flip_lh)],
        )
    task(
        ("yl", 1, 0), deps=[("norm",)], prio=1, takes=[y_take("yl", 1, 0)],
        pushes=[y_copy("yr", 1, 1, 0, "n", flip_lh)] + z_first(1, 1),
    )
    task(("yn", 1, 0), deps=[("norm",)], prio=2, takes=[y_take("yn", 1, 0)], pushes=z_first(1, 2))
    task(("yr", 1, 0), deps=[("norm",)], prio=2, takes=[y_take("yr", 1, 0)], pushes=z_first(1, 3))
    task(("w", "i", 1), deps=[("z", 0, 0, 1, 1), ("w", "i", 0)], prio=3, pushes=[w_push("i", 1)])
    for w in ("q", "i"):
        task(
            ("w", w), deps=[("norm",), ("w", w, 1)], prio=2,
            takes=[w_take(w, 0), w_take(w, 1)], pushes=x_push(w, 1),
        )
        x_relay(w, 0, [("norm",)])
        x_relay(w, 1, [("w", w)])
    n = len(CHUNKS)
    for c in range(n):
        pair = (("o", c), ("m", c))
        if c == 0:
            after = [("z", 0, 0, 1, 3), ("z", 0, 0, -1, 3)]
        else:
            after = [("w2s", c - 1)] + ([("w2p", c - 2)] if c >= 2 else [])
        task(("w2s", c), deps=after, prio=6, pushes=[w_push(w) for w in pair])
        if c == 0:
            after = [("x", "i", 0, 1), ("x", "i", 0, -1), ("w", "i"), ("x", "q", 1, 1), ("x", "q", 1, -1)]
        else:
            after = [("w2q", c - 1)] + ([("x", "i", 1, 1), ("x", "i", 1, -1)] if c == 1 else [])
            for lag, qs in LAGS:
                if c >= lag:
                    after += [("x", (w, c - lag), q, d) for w in "om" for q in qs for d in (1, -1)]
        task(("w2p", c), deps=after, prio=7, pushes=x_push(pair[0], 0) + x_push(pair[1], 0))
        task(
            ("w2q", c), deps=[("w2s", c), ("w2p", c)], prio=7, takes=[w_take(w) for w in pair],
            pushes=x_push(pair[0], 1) + x_push(pair[1], 1),
        )
        for w in pair:
            x_relay(w, 0, [("w2p", c)])
            x_relay(w, 1, [("w2q", c)])
    first_relays = [t.name for t in tasks if t.name[0] in ("z", "z4", "yl", "yn", "yr", "w")]
    first_relays += [("x", w, q, d) for w in ("q", "i") for q in range(2) for d in (1, -1)]

    groups = ((0,), (1, -1), (2, -2), (3, -3), (4,))

    def rows_of(dzs):
        return [pl.ds(pl.multiple_of(zn[dz % NZ] * 128, 128), 128) for dz in dzs]

    def product(lhs, weights, h):
        cols = pl.ds(h * HALF, HALF)
        rhs = weights[..., cols].reshape(384, HALF)
        return lax.dot_general(lhs, rhs, NT, preferred_element_type=F32)

    def project(dzs):
        if dzs == (0,):
            for copy in local_copies[:2]:
                copy.wait()
        rows = rows_of(dzs)
        acc_q = jnp.zeros((128 * len(dzs), 384), F32)
        acc_m = jnp.zeros((128 * len(dzs), 384), F32)
        for h in range(2):
            for q in (yl, nl):
                lhs = jnp.concatenate([xg[h, q, r] for r in rows], axis=0)
                acc_q += product(lhs, WQ.at[q], h)
                if q is yl:
                    acc_m += product(lhs, WM.at[q], h)
        for i, r in enumerate(rows):
            hq[r] = acc_q[i * 128 : (i + 1) * 128]
            hm[r] = acc_m[i * 128 : (i + 1) * 128]

    def project_last(dzs):
        rows = rows_of(dzs)
        acc = jnp.concatenate([hm[r] for r in rows], axis=0)
        for h in range(2):
            acc += product(jnp.concatenate([xg[h, nl, r] for r in rows], axis=0), WM.at[nl], h)
        for i, r in enumerate(rows):
            hm[r] = acc[i * 128 : (i + 1) * 128]

    def to_partner(kind, dz):
        src, dst = (hq, hxq) if kind == "hq" else (hm, hxm)
        zz = zn[dz % NZ]
        there = pl.ds(pl.multiple_of(lax.rem(zz, NZ // 2) * 128, 128), 128)
        return zz // (NZ // 2), src.at[rows_of((dz,))[0]], dst.at[there]

    def send_sums(kind, dzs):
        for dz in dzs:
            owner, src, dst = to_partner(kind, dz)
            i = index.setdefault((kind, dz), len(index))
            copy = pltpu.make_async_remote_copy(
                src_ref=src, dst_ref=dst, send_sem=send.at[i], recv_sem=recv.at[i],
                device_id=partner, device_id_type=MESH,
            )
            pl.when(owner == nk)(copy.start)
            sums_sent.append((owner, copy))

    def take_sums(kind):
        for dzs in groups:
            for dz in dzs:
                owner, _, dst = to_partner(kind, dz)
                i = index[(kind, dz)]
                copy = pltpu.make_async_remote_copy(
                    src_ref=dst, dst_ref=dst, send_sem=send.at[i], recv_sem=recv.at[i],
                    device_id=partner, device_id_type=MESH,
                )
                pl.when(owner == k)(copy.wait_recv)

    sums_sent = []
    k_scale = LINK_RATE / 600e3
    early = x_last("q") + [t for t in x_last("i") if t[0][2] == 0]
    late = [t for t in x_last("i") if t[0][2] == 1]
    early_relays = [("x", w, q, d) for w, q in (("q", 0), ("q", 1), ("i", 0)) for d in (1, -1)]
    late_relays = [("x", "i", 1, d) for d in (1, -1)]
    for g, dzs in enumerate(groups):
        takes, deps = (list(early), list(early_relays)) if g == 0 else ([], [("p", g - 1)])
        for dz in dzs:
            takes += [y_take(kind, 0, dz) for kind in ("yn", "yr")]
            deps += [("yl", 0, dz % NZ)]
            if dz == 0:
                deps += [("norm",), ("yl", 1, 0), ("yn", 1, 0), ("yr", 1, 0)]
            elif dz == 4:
                deps += [("z4",)]
                takes += [z_take(1, r, d, 4) for r in range(4) for d in (1, -1)]
            else:
                d = -1 if dz > 0 else 1
                deps += [("z", 0, 0, d, abs(dz))] + [("z", 1, r, d, abs(dz)) for r in range(4)]
        task(
            ("p", g), takes=takes, deps=deps, body=lambda dzs=dzs: (project(dzs), send_sums("hq", dzs)),
            prio=30, work=0.9 if len(dzs) == 1 else 1.4, pushes=[(("hq", g), "k", 100e3 * k_scale, None)],
        )
        task(
            ("pl", g), takes=late if g == 0 else [],
            deps=late_relays + [("p", 0)] if g == 0 else [("pl", g - 1), ("p", g)],
            body=lambda dzs=dzs: (project_last(dzs), send_sums("hm", dzs)), prio=31,
            work=0.5 if len(dzs) == 1 else 0.67, pushes=[(("hm", g), "k", 100e3 * k_scale, None)],
        )

    def head_norm(values, gain):
        centred = values - jnp.mean(values, -1, keepdims=True)
        spread = jnp.mean(centred * centred, -1, keepdims=True)
        return (centred * lax.rsqrt(spread + EPS) * gain[...].astype(F32)).astype(BF16)

    def own_rows(i):
        return pl.ds(pl.multiple_of(k * 512 + i * IMAGE, IMAGE), IMAGE)

    def attend(i):
        mine = pl.ds(i * IMAGE, IMAGE)
        joined = hq[own_rows(i)] + hxq[mine]
        q = head_norm(joined[:, 0:128], q_gain)
        kk = head_norm(joined[:, 128:256], k_gain)
        v = joined[:, 256:384].astype(BF16)
        scores = lax.dot_general(q, kk, NT, preferred_element_type=F32) * HD ** (-0.5)
        e = jnp.exp(scores - jnp.max(scores, -1, keepdims=True))
        probs = (e / jnp.sum(e, -1, keepdims=True)).astype(BF16)
        attended = jnp.dot(probs, v, preferred_element_type=F32)
        att[k, mine, pl.ds(0, 128)] = attended.astype(BF16)

    def activate(i):
        mine = pl.ds(i * IMAGE, IMAGE)
        unit = (lax.broadcasted_iota(jnp.int32, (IMAGE, 128), 1) == 0).astype(F32).astype(BF16)
        pre = hm[own_rows(i)] + hxm[mine] + lax.dot_general(
            unit, BI[...].reshape(384, 128), NT, preferred_element_type=F32
        )
        hidden = 0.5 * pre * (1.0 + lax.erf(pre * (0.5 ** 0.5)))
        att[k, mine, pl.ds(128, 384)] = hidden.astype(BF16)

    def att_refs(i):
        ref = att.at[k, pl.ds(i * IMAGE, IMAGE)]
        return ref, ref, partner

    for i in range(2):
        task(
            ("attend", i), deps=first_relays + [("pl", 4)] + [("attend", 0)] * i, prio=10, work=0.45,
            takes=[(("hq", g), None) for g in range(5)] if i == 0 else [],
            body=lambda i=i: (take_sums("hq") if i == 0 else None, attend(i)),
        )
    for i in range(2):
        takes = []
        if i == 0:
            takes = [(("bias", d), lambda d=d: BI.at[xs[-d % NX]]) for d in (1, -1, 2)]
            takes += [(("hm", g), None) for g in range(5)]
        task(
            ("image", i), takes=takes, deps=[("attend", 1)] + [("image", 0)] * i, prio=10, work=0.45,
            body=lambda i=i: (take_sums("hm") if i == 0 else None, activate(i)),
            pushes=[(("att", i), "k", 256 * 512 * 2 * k_scale, lambda i=i: att_refs(i))],
        )

    def output_terms(c, half):
        if c == 0 and half == 0:
            for copy in local_copies[2:]:
                copy.wait()
        _, c0, width = CHUNKS[c]
        who = k if half == 0 else nk
        cols = slice(c0, c0 + width)
        for i in range(2):
            row = pl.multiple_of(who * 512 + i * 256, 256)
            a = att[who, pl.ds(i * 256, 256)]
            for q in range(2):
                part[q, pl.ds(row, 256), pl.ds(c0, width)] = jnp.dot(
                    a[:, :128], OW[q, :, :, cols].reshape(128, width), preferred_element_type=F32
                ) + jnp.dot(
                    a[:, 128:], MO[q, :, :, cols].reshape(384, width), preferred_element_type=F32
                )

    for c, (_, _, width) in enumerate(CHUNKS):
        pair = (("o", c), ("m", c))
        for half in range(2):
            deps = [("image", 1)]
            deps += [("x", w, q, d) for w in pair for q in range(2) for d in (1, -1)]
            deps += [("terms", c, 0)] if half else []
            deps += [("terms", c - 1, 1)] if c else []
            takes = (x_last(pair[0]) + x_last(pair[1])) if half == 0 else []
            if c == 0 and half == 1:
                takes = [
                    (("att", i), lambda i=i: att.at[nk, pl.ds(i * IMAGE, IMAGE)]) for i in range(2)
                ]
            task(
                ("terms", c, half), takes=takes, deps=deps, prio=9, work=1.44 * width / 768,
                body=lambda c=c, half=half: output_terms(c, half),
            )

    half = BLOCK // 2

    def term(c, r, dz):
        row = pl.multiple_of((zn[dz % NZ] * 2 + rel_h[r]) * BLOCK, BLOCK)
        return part.at[rel_l[r], pl.ds(row, BLOCK), pl.ds(*CHUNKS[c][1:])]

    def reduction(c):
        kind, _, width = CHUNKS[c]
        zs, zr, ns, nr, ms, mr = chunk_refs[6 * c : 6 * c + 6]
        block, groups = BLOCK * width * 2, (1 if kind == "y" else 4)
        work = 0.05 + 0.12 * width / HALF
        ready = ("terms", c, 1)

        def along_z(g, r, d, dist):
            slot, landing = zs.at[g, 0 if d == 1 else 1, dist - 1], zr.at[g, 0 if d == 1 else 1, dist - 1]
            if dist == 4:
                slot, landing = slot.at[pl.ds(0, half)], landing.at[pl.ds(0, half)]
            before = zr.at[g, 0 if d == 1 else 1, min(dist, 3)]
            if dist == 3:
                before = before.at[pl.ds(0, half)]
            lo = 0 if d == 1 else half

            def body():
                blk = term(c, r, d * dist)
                if dist == 4:
                    slot[...] = blk[pl.ds(lo, half)].astype(BF16)
                elif dist == 3:
                    slot[pl.ds(half - lo, half)] = blk[pl.ds(half - lo, half)].astype(BF16)
                    slot[pl.ds(lo, half)] = (
                        blk[pl.ds(lo, half)] + before[...].astype(F32)
                    ).astype(BF16)
                else:
                    slot[...] = (blk[...] + before[...].astype(F32)).astype(BF16)

            from_y = ("y_end", c, (d * dist) % NZ) if kind == "y" else ready
            prio = 3 if kind == "y" else 8 - dist * 0.5 + (0 if r in (2, 3) else 0.3)
            task(
                ("c", c, r, d, dist), body=body, work=work, prio=prio + c * 0.01,
                takes=[] if dist == 4 else [(("c", c, r, d, dist + 1), lambda: before)],
                deps=[from_y] + ([] if dist == 4 else [("c", c, r, d, dist + 1)]),
                pushes=[
                    (("c", c, r, d, dist), ("z", d), block // 2 if dist == 4 else block,
                     lambda: (slot, landing, at_z(d)))
                ],
            )

        def z_end(g, r):
            def body():
                blk = term(c, r, 0)
                blk[...] = blk[...] + zr[g, 0, 0].astype(F32) + zr[g, 1, 0].astype(F32)
            task(
                ("z_end", c, r), body=body, work=work, prio=2,
                takes=[(("c", c, r, d, 1), lambda i=i: zr.at[g, i, 0]) for i, d in enumerate((1, -1))],
                deps=[("c", c, r, d, 1) for d in (1, -1)] + ([("y_end", c, 0)] if kind == "y" else []),
            )

        def along_y(g, dz, deps_out, deps_mid, deps_end, prios):
            tree = (c + dz) % 2
            far, near = ((flip_lh, "n"), (flip_l, "l")) if tree == 0 else ((flip_l, "l"), (flip_lh, "n"))
            direct, mid = (2, 1) if tree == 0 else (1, 2)

            def out_body():
                for j, r in enumerate((direct, 3)):
                    ns[g, j] = term(c, r, dz)[...].astype(BF16)

            def mid_body():
                ms[g] = (term(c, mid, dz)[...] + nr[g, 1].astype(F32)).astype(BF16)

            def end_body():
                blk = term(c, 0, dz)
                blk[...] = blk[...] + nr[g, 0].astype(F32) + mr[g].astype(F32)

            task(
                ("y_out", c, dz), body=out_body, deps=deps_out(direct), prio=prios[0],
                work=0.05 + 0.15 * width / HALF,
                pushes=[
                    (("n", c, dz, j), far[1], block, lambda j=j: (ns.at[g, j], nr.at[g, j], far[0]))
                    for j in (1, 0)
                ],
            )
            task(
                ("y_mid", c, dz), body=mid_body, work=work, prio=prios[1],
                takes=[(("n", c, dz, 1), lambda: nr.at[g, 1])],
                deps=[("y_out", c, dz)] + deps_mid(mid),
                pushes=[(("m", c, dz), near[1], block, lambda: (ms.at[g], mr.at[g], near[0]))],
            )
            task(
                ("y_end", c, dz), body=end_body, work=work, prio=prios[2],
                takes=[(("n", c, dz, 0), lambda: nr.at[g, 0]), (("m", c, dz), lambda: mr.at[g])],
                deps=[("y_mid", c, dz)] + deps_end,
            )

        if kind == "y":
            for dz in range(NZ):
                far = min(dz, NZ - dz)
                along_y(
                    dz, dz, lambda r: [ready], lambda r: [], [],
                    (20 - far, 4 - far * 0.1, 5 - far * 0.1),
                )
        for g in range(groups):
            for d in (1, -1):
                for dist in (4, 3, 2, 1):
                    along_z(g, g, d, dist)
            z_end(g, g)
        if kind == "z":
            along_y(
                0, 0, lambda r: [("z_end", c, r), ("z_end", c, 3)], lambda r: [("z_end", c, r)],
                [("z_end", c, 0)], (1, 1, 1),
            )

    for c in range(n):
        reduction(c)

    assert sorted(ORDER) == list(range(len(tasks)))
    for step in [tasks[i] for i in ORDER]:
        for key, ref in step.takes:
            if ref is not None:
                take(key, ref())
        if step.body is not None:
            step.body()
        for key, _, _, refs in step.pushes:
            if refs is not None:
                push(key, *refs())

    own = pl.ds(pl.multiple_of((z * 2 + yh) * BLOCK, BLOCK), BLOCK)
    g = out_bias[...].astype(F32)
    out[...] = part[yl, own] + jnp.concatenate([g[i : i + 1] for i in range(PIECE // 128)], axis=1)
    for copy in started:
        copy.wait_send()
    for owner, copy in sums_sent:
        pl.when(owner == nk)(copy.wait_send)
    assert len(index) <= N_SEMS, len(index)


def per_device(
    tokens, ln_gain, qkv_weight, q_gain, k_gain, out_weight, mlp_in, mlp_bias, mlp_out, out_bias
):
    wq = jnp.transpose(qkv_weight, (1, 2, 3, 0))
    wm = jnp.transpose(mlp_in).reshape(2, UNITS, PIECE)
    mo = mlp_out.reshape(2, UNITS, PIECE)
    vm, hbm = pl.BlockSpec(memory_space=pltpu.VMEM), pl.BlockSpec(memory_space=pltpu.HBM)
    scratch = [
        pltpu.VMEM((BLOCK, PIECE), BF16),
        pltpu.VMEM((8, 128), F32),
        pltpu.VMEM((3, 8, 128), F32),
        pltpu.VMEM((2, 2, ROWS, HALF), BF16),
        pltpu.VMEM((2, 3, NX, 32, PIECE), BF16),
        pltpu.VMEM((2, NX, UNITS, PIECE), BF16),
        pltpu.VMEM((256, 128), BF16),
        pltpu.VMEM((NX, UNITS, 128), BF16),
        pltpu.VMEM((2, NX, 32, PIECE), BF16),
        pltpu.VMEM((2, NX, UNITS, PIECE), BF16),
        pltpu.VMEM((ROWS, 384), F32),
        pltpu.VMEM((ROWS, 384), F32),
        pltpu.VMEM((512, 384), F32),
        pltpu.VMEM((512, 384), F32),
        pltpu.VMEM((2, 512, 512), BF16),
        pltpu.VMEM((2, ROWS, PIECE), F32),
    ]
    for kind, _, width in CHUNKS:
        block = (BLOCK, width)
        groups, ys = (1, NZ) if kind == "y" else (4, 1)
        scratch += [pltpu.VMEM((groups, 2, 4, *block), BF16)] * 2
        scratch += [pltpu.VMEM((ys, 2, *block), BF16)] * 2
        scratch += [pltpu.VMEM((ys, *block), BF16)] * 2
    scratch += [
        pltpu.SemaphoreType.DMA((N_SEMS,)),
        pltpu.SemaphoreType.DMA((N_SEMS,)),
        pltpu.SemaphoreType.DMA((5,)),
    ]
    sums = pl.pallas_call(
        kernel,
        out_shape=jax.ShapeDtypeStruct((BLOCK, PIECE), F32),
        in_specs=[hbm, vm, hbm, hbm, vm, vm, hbm, vm, hbm, vm],
        out_specs=vm,
        scratch_shapes=scratch,
        compiler_params=pltpu.CompilerParams(
            collective_id=0, has_side_effects=True, vmem_limit_bytes=60 * 1024 * 1024
        ),
        name="layer",
    )(
        tokens, ln_gain.reshape(PIECE // 128, 128), wq, wm, q_gain.reshape(1, HD),
        k_gain.reshape(1, HD), out_weight, mlp_bias, mo,
        out_bias.reshape(PIECE // 128, 128),
    )
    return tokens.astype(F32) + sums


def solution(mesh):
    split = Mesh(
        mesh.devices.reshape(NX, 2, 2, NZ, 2), ("x", "yl", "k", "z", "yh")
    )
    token_axes, row, col = ("x", "z", "yh"), ("yl", "k"), ("z", "yh")
    placed = (
        P(token_axes, row),
        P(row),
        P(row, None, col, "x"),
        P(),
        P(),
        P(col, "x", row),
        P(row, token_axes),
        P(token_axes),
        P(token_axes, row),
        P(row),
    )
    return jax.shard_map(
        per_device, mesh=split, in_specs=placed, out_specs=P(token_axes, row), check_vma=False
    )
```
